32 devices in a mesh: blk: 8 (over z, x), uly: 4 (over y, core).
Axes of the slice: x: 2, y: 2, z: 4, core: 2. Of those that a mesh axis runs over, the one named last changes fastest.
Arguments:
- q_raw: bfloat16 [1152, 24, 128], P('blk', 'uly'), may hold values from -120 to 120
- k_raw: bfloat16 [1152, 24, 128], P('blk', 'uly'), may hold values from -120 to 120
- values: bfloat16 [1152, 24, 128], P('blk', 'uly'), may hold values from -6 to 6
- out_grad: bfloat16 [1152, 24, 128], P('blk', 'uly'), may hold values from -16 to 16
- q_gain: float32 [2, 128], replicated, may hold values from 0.5 to 6.5
- k_gain: float32 [2, 128], replicated, may hold values from 0.5 to 6.5
Outputs:
- q_grad: bfloat16 [1152, 24, 128], P('blk', 'uly')
- k_grad: bfloat16 [1152, 24, 128], P('blk', 'uly')
- v_grad: bfloat16 [1152, 24, 128], P('blk', 'uly')
- q_gain_grad: float32 [2, 128], replicated
- k_gain_grad: float32 [2, 128], replicated
The draws below stay inside these ranges and needn't reach their ends.
All inputs are finite; a program needn't handle non-finite values.
Results may differ from the reference program's by a relative error of at most 0.009.
The reference program's roundings to bfloat16 on the way (of `probs_low`) count: a program that leaves them out, or rounds other values in their place, can miss the bound.
Values may be sent and summed in bfloat16 or wider, within the bound.
A program may use at most 64 MiB of HBM per device.

```python
import math
import jax
import jax.numpy as jnp
from jax import lax

HEADS = 24
HD = 128
TXT = 512
SEQ = 1152


def scaled_normal(key, shape):
    noise_key, row_key, col_key = jax.random.split(key, 3)
    base = jnp.clip(jax.random.normal(noise_key, shape, jnp.float32), -6.0, 6.0)
    row_scale = jnp.exp(jax.random.uniform(row_key, (shape[0], shape[1], 1), jnp.float32, 0.0, math.log(10.0)))
    col_scale = jnp.exp(jax.random.uniform(col_key, (1, 1, shape[2]), jnp.float32, math.log(0.5), math.log(2.0)))
    return base * row_scale * col_scale


def raw_pair(key):
    base_key = jax.random.fold_in(key, 101)
    split_keys = jax.random.split(base_key, 2)
    shape = (SEQ, HEADS, HD)
    queries = scaled_normal(split_keys[0], shape)
    key_rows = scaled_normal(split_keys[1], shape)
    return (jnp.clip(queries, -120.0, 120.0), jnp.clip(key_rows, -120.0, 120.0))


def draw_q_raw(key, part):
    return raw_pair(key)[0].astype(jnp.bfloat16)


def draw_k_raw(key, part):
    return raw_pair(key)[1].astype(jnp.bfloat16)


def draw_out_grad(key, part):
    local_key = jax.random.fold_in(key, 202)
    position = jnp.arange(SEQ).astype(jnp.float32)
    rising = (1.0 + 2.0 * position / SEQ)[:, None, None]
    base = jnp.clip(jax.random.normal(local_key, (SEQ, HEADS, HD), jnp.float32), -5.0, 5.0) * rising
    return base.astype(jnp.bfloat16)


def gain_draw(key, salt):
    local_key = jax.random.fold_in(key, salt)
    return jnp.exp(jax.random.uniform(local_key, (2, HD), jnp.float32, math.log(0.5), math.log(2.0)))


def draw_q_gain(key, part):
    return gain_draw(key, 303)


def draw_k_gain(key, part):
    return gain_draw(key, 404)


def levels(key, shape, cuts, least, top_value):
    level = 1.0
    for dim, blocks in cuts:
        steps = jax.random.uniform(jax.random.fold_in(jax.random.fold_in(key, 6), dim), (blocks,), jnp.float32, least / len(cuts), top_value / len(cuts))
        level = level * jnp.repeat(jnp.exp(steps), shape[dim] // blocks).reshape((-1,) + (1,) * (len(shape) - 1 - dim))
    return level


def gaussian(stream_key, shape, spread, limit, cuts=(), kind=jnp.bfloat16):
    entries = jax.random.normal(stream_key, shape, jnp.float32) * spread
    if len(cuts) > 0:
        entries = levels(stream_key, shape, cuts, -0.22, 0.18) * entries
    return jnp.clip(entries, min=-limit, max=limit).astype(kind)


def setup_inputs(seed: int = 0) -> dict:
    key_list = jax.random.split(jax.random.key(seed), 7)
    q_raw = draw_q_raw(jax.random.fold_in(key_list[6], 71), 0)
    k_raw = draw_k_raw(jax.random.fold_in(key_list[6], 71), 0)
    values = gaussian(key_list[2], (SEQ, HEADS, HD), 1.0, 6.0, ((0, 8), (1, 4)))
    out_grad = draw_out_grad(jax.random.fold_in(key_list[6], 71), 0)
    q_gain = draw_q_gain(jax.random.fold_in(key_list[6], 71), 0)
    k_gain = draw_k_gain(jax.random.fold_in(key_list[6], 71), 0)
    return dict(q_raw=q_raw, k_raw=k_raw, values=values, out_grad=out_grad, q_gain=q_gain, k_gain=k_gain)


epsilon = 1e-06

def gain_rows(gain, position):
    return jnp.where((position < TXT)[:, None], gain[0][None, :], gain[1][None, :])

def normalize(raw, gains):
    widened = raw.astype(jnp.float32)
    root_mean = jnp.sqrt(lax.optimization_barrier(jnp.mean(widened * widened, axis=-1, keepdims=True)) + epsilon)
    unit = widened / root_mean
    return (unit, root_mean, (unit * gains[:, None, :]).astype(jnp.bfloat16))

def norm_back(grad_norm, unit, root_mean, gains):
    grad_unit = grad_norm * gains[:, None, :]
    return (grad_unit - unit * lax.optimization_barrier(jnp.mean(grad_unit * unit, axis=-1, keepdims=True))) / root_mean

def gain_parts(grad_norm, unit, position):
    per_row = lax.optimization_barrier(jnp.sum(grad_norm * unit, axis=1))
    text_rows = (position < TXT)[:, None]
    return jnp.stack([lax.optimization_barrier(jnp.sum(jnp.where(text_rows, per_row, 0.0), axis=0)), lax.optimization_barrier(jnp.sum(jnp.where(text_rows, 0.0, per_row), axis=0))])

def heads_first(array):
    return jnp.transpose(array, (1, 0, 2))

def reference(q_raw, k_raw, values, out_grad, q_gain, k_gain):
    position = jnp.arange(SEQ, dtype=jnp.int32)
    factor = 1.0 / math.sqrt(HD)
    q_gains = gain_rows(q_gain, position)
    k_gains = gain_rows(k_gain, position)
    q_unit, q_root, q_norm = normalize(q_raw, q_gains)
    k_unit, k_root, k_norm = normalize(k_raw, k_gains)

    def per_head(members):
        q_head, k_head, v_head, g_head = members
        head_scores = jnp.dot(q_head, k_head.T, preferred_element_type=jnp.float32) * factor
        peak = lax.optimization_barrier(jnp.max(head_scores, axis=1, keepdims=True))
        log_total = peak + jnp.log(lax.optimization_barrier(jnp.sum(jnp.exp(head_scores - peak), axis=1, keepdims=True)))
        probs = jnp.exp(head_scores - log_total)
        probs_low = probs.astype(jnp.bfloat16)
        attn = jnp.dot(probs, v_head.astype(jnp.float32), precision=lax.Precision.HIGHEST, preferred_element_type=jnp.float32)
        row_dot = lax.optimization_barrier(jnp.sum(g_head.astype(jnp.float32) * attn, axis=1, keepdims=True))
        grad_probs = jnp.dot(g_head, v_head.T, preferred_element_type=jnp.float32)
        mixed = (probs * grad_probs).astype(jnp.bfloat16)
        weighted_grad = jnp.dot(mixed, k_head, preferred_element_type=jnp.float32)
        weighted_keys = jnp.dot(probs_low, k_head, preferred_element_type=jnp.float32)
        grad_query = factor * (weighted_grad - row_dot * weighted_keys)
        grad_scores = (probs * (grad_probs - row_dot)).astype(jnp.bfloat16)
        grad_key = factor * jnp.dot(grad_scores.T, q_head, preferred_element_type=jnp.float32)
        grad_value = jnp.dot(probs_low.T, g_head, preferred_element_type=jnp.float32)
        return (grad_query, grad_key, grad_value)
    grad_query, grad_key, grad_value = lax.map(per_head, (heads_first(q_norm), heads_first(k_norm), heads_first(values), heads_first(out_grad)))
    grad_q_norm = heads_first(grad_query)
    grad_k_norm = heads_first(grad_key)
    v_grad = heads_first(grad_value).astype(jnp.bfloat16)
    q_grad = norm_back(grad_q_norm, q_unit, q_root, q_gains).astype(jnp.bfloat16)
    k_grad = norm_back(grad_k_norm, k_unit, k_root, k_gains).astype(jnp.bfloat16)
    q_gain_grad = gain_parts(grad_q_norm, q_unit, position)
    k_gain_grad = gain_parts(grad_k_norm, k_unit, position)
    return (q_grad, k_grad, v_grad, q_gain_grad, k_gain_grad)
```

```python
import functools
import math

import jax
import jax.numpy as jnp
from jax import lax
from jax.experimental import pallas as pl
from jax.experimental.pallas import tpu as pltpu
from jax.sharding import PartitionSpec as P

TXT = 512
EPS = 1e-06
LANES = 128
CHUNK = 256
KEYS = 1152
MESH = pl.DeviceIdType.MESH
f32, bf16 = jnp.float32, jnp.bfloat16


def partner(me, step, n):
    if n & (n - 1):
        return (me + step) % n
    out, bit = 0, 1
    while bit < n:
        out = out + ((me // bit + step // bit) % 2) * bit
        bit *= 2
    return out


def kernel(
    n, n_uly, heads, rows,
    k_hbm, v_hbm, q_hbm, g_hbm, qg_hbm, kg_hbm,
    dq_out, dk_out, dv_out, q_gain_out, k_gain_out,
    k_in, v_in, q_in, g_in,
    k_all, v_all, q_all, g_all, kn, kn_t, dk_acc, dv_acc, dq_buf, dk_buf, dv_buf,
    weights_buf, grad_buf, low_buf, mixed_buf, scores_grad_buf, peaks, sums, dots, scales,
    qg_ref, kg_ref, gain_mine, gain_heads, gain_group, gain_uly,
    staged, in_send, in_recv, back_send, back_recv, g1_send, g1_recv, g2_send, g2_recv,
):
    me = lax.axis_index("blk")
    uly = lax.axis_index("uly")
    total = n * rows
    full = total // CHUNK
    tail = total - full * CHUNK
    tiles = total // LANES
    width = k_in.shape[2]
    factor = 1.0 / math.sqrt(width)
    factor2 = factor * math.log2(math.e)
    keys = max(d for d in range(LANES, min(total, KEYS) + 1, LANES) if total % d == 0)
    phase = (uly % 2) * (heads % n)

    def head_of(dev):
        return (heads * dev + phase) // n

    def owns(dev):
        return (heads * dev + phase) % n + heads >= n

    def owner(h):
        return ((h + 1) * n - phase + heads - 1) // heads - 1

    mine = head_of(me)
    i_own = owns(me)

    sources = (k_hbm, v_hbm, q_hbm, g_hbm)
    ins = (k_in, v_in, q_in, g_in)
    alls = (k_all, v_all, q_all, g_all)
    backs = (dq_buf, dk_buf, dv_buf)
    outs = (dq_out, dk_out, dv_out)

    def block(dev):
        return pl.ds(pl.multiple_of(dev * rows, 16), rows)

    def stage(a):
        return pltpu.make_async_copy(sources[a], ins[a], staged.at[a])

    gain_stages = (
        pltpu.make_async_copy(qg_hbm, qg_ref, staged.at[4]),
        pltpu.make_async_copy(kg_hbm, kg_ref, staged.at[5]),
    )

    barrier = pltpu.get_barrier_semaphore()
    for s in range(1, n):
        pl.semaphore_signal(
            barrier, inc=1, device_id={"blk": partner(me, s, n)}, device_id_type=MESH
        )
    for s in range(1, n_uly):
        pl.semaphore_signal(
            barrier, inc=1, device_id={"uly": (uly + s) % n_uly}, device_id_type=MESH
        )
    for a in range(4):
        stage(a).start()
    for copy in gain_stages:
        copy.start()
    pl.semaphore_wait(barrier, n - 1 + n_uly - 1)

    def in_copy(a, s, h, dev):
        return pltpu.make_async_remote_copy(
            src_ref=ins[a].at[h], dst_ref=alls[a].at[block(me)],
            send_sem=in_send.at[a, s], recv_sem=in_recv.at[a, me],
            device_id={"blk": dev}, device_id_type=MESH,
        )

    def send_in(a, s):
        dev = partner(me, s, n)

        @pl.when(owns(dev))
        def _():
            in_copy(a, s, head_of(dev), dev).start()

    def keep_in(a):
        @pl.when(i_own)
        def _():
            pltpu.make_async_copy(
                ins[a].at[mine], alls[a].at[block(me)], in_recv.at[a, me]
            ).start()

    def wait_in(a, src):
        pltpu.make_async_copy(ins[a].at[0], alls[a].at[block(src)], in_recv.at[a, src]).wait()

    for a in (0, 1):
        stage(a).wait()
        for s in range(n - 1, 0, -1):
            send_in(a, s)
    for a in (2, 3):
        stage(a).wait()
    for copy in gain_stages:
        copy.wait()
    for a in range(4):
        keep_in(a)
    for s in range(1, n):
        for a in (2, 3):
            send_in(a, s)

    def back_copy(a, dev):
        return pltpu.make_async_remote_copy(
            src_ref=backs[a].at[block(dev)], dst_ref=outs[a].at[mine],
            send_sem=back_send.at[a, dev], recv_sem=back_recv.at[a, mine],
            device_id={"blk": dev}, device_id_type=MESH,
        )

    def send_back(a, dev):
        @pl.when(dev != me)
        def _():
            back_copy(a, dev).start()

        @pl.when(dev == me)
        def _():
            pltpu.make_async_copy(
                backs[a].at[block(dev)], outs[a].at[mine], back_recv.at[a, mine]
            ).start()

    def gain_copy(dev):
        return pltpu.make_async_remote_copy(
            src_ref=gain_mine, dst_ref=gain_heads.at[mine],
            send_sem=g1_send.at[dev], recv_sem=g1_recv.at[mine],
            device_id={"blk": dev}, device_id_type=MESH,
        )

    def uly_copy(s):
        return pltpu.make_async_remote_copy(
            src_ref=gain_group, dst_ref=gain_uly.at[uly],
            send_sem=g2_send.at[s], recv_sem=g2_recv.at[uly],
            device_id={"uly": (uly + s) % n_uly}, device_id_type=MESH,
        )

    def gains_at(gain_ref, base, size):
        position = base + lax.broadcasted_iota(jnp.int32, (size, width), 0)
        text = position < TXT
        return text, jnp.where(text, gain_ref[0:1, :], gain_ref[1:2, :])

    def unit_of(raw):
        wide = raw.astype(f32)
        inverse = lax.rsqrt(jnp.mean(wide * wide, axis=-1, keepdims=True) + EPS)
        return wide * inverse, inverse

    def finish(grad, unit, inverse, text, gains):
        part = grad * unit
        scaled = grad * gains
        text_sum = jnp.sum(jnp.where(text, part, 0.0), axis=0, keepdims=True)
        image_sum = jnp.sum(jnp.where(text, 0.0, part), axis=0, keepdims=True)
        result = (scaled - unit * jnp.mean(scaled * unit, axis=-1, keepdims=True)) * inverse
        return result.astype(bf16), text_sum, image_sum

    @pl.when(i_own)
    def _():
        low = me < n // 2
        turn = jnp.where(low, me, n - 1 - me) >= n // 4
        half = full // 2
        half_need = (CHUNK * half - 1) // rows + 1
        half_done = (CHUNK * half) // rows
        rest_done = (CHUNK * (full - half)) // rows
        nt = (((1,), (1,)), ((), ()))

        def real(i, count):
            return jnp.where(low, i, count - 1 - i)

        gain_mine[...] = jnp.zeros_like(gain_mine)
        dk_acc[...] = jnp.zeros_like(dk_acc)
        dv_acc[...] = jnp.zeros_like(dv_acc)

        @pl.loop(0, n)
        def _(src):
            wait_in(0, src)

        @pl.loop(0, tiles)
        def _(c):
            at = pl.ds(pl.multiple_of(c * LANES, LANES), LANES)
            text, gains = gains_at(kg_ref, c * LANES, LANES)
            unit, _inverse = unit_of(k_all[at, :])
            normed = unit * gains
            kn[at, :] = normed.astype(bf16)
            kn_t[:, at] = normed.T.astype(bf16)

        @pl.loop(0, n)
        def _(src):
            wait_in(1, src)

        def over_keys(body):
            if keys == total:
                body(0)
            else:
                @pl.loop(0, total // keys)
                def _(j):
                    body(j)

        def attend(start, size):
            start = pl.multiple_of(start, LANES)
            at = pl.ds(start, size)
            text, gains = gains_at(qg_ref, start, size)
            unit, inverse = unit_of(q_all[at, :])
            qn = (unit * gains).astype(bf16)
            grads = g_all[at, :]
            cols = pl.ds(0, size)
            per = keys // LANES

            def first(j):
                base = pl.multiple_of(j * keys, LANES)
                rng = pl.ds(base, keys)
                scores = lax.dot_general(kn[rng, :], qn, nt, preferred_element_type=f32)
                grad_probs = lax.dot_general(v_all[rng, :], grads, nt, preferred_element_type=f32)
                for b in range(per):
                    part = slice(b * LANES, (b + 1) * LANES)
                    here = pl.ds(base + b * LANES, LANES)
                    row = pl.ds(j * per + b, 1)
                    peak = jnp.max(scores[part], axis=0, keepdims=True)
                    weights = jnp.exp2((scores[part] - peak) * factor2)
                    peaks[row, cols] = peak
                    sums[row, cols] = jnp.sum(weights, axis=0, keepdims=True)
                    dots[row, cols] = jnp.sum(weights * grad_probs[part], axis=0, keepdims=True)
                    weights_buf[here, cols] = weights
                    grad_buf[here, cols] = grad_probs[part]

            over_keys(first)
            peak_all = peaks[:, cols]
            lift = jnp.exp2((peak_all - jnp.max(peak_all, axis=0, keepdims=True)) * factor2)
            inverse_total = 1.0 / jnp.sum(lift * sums[:, cols], axis=0, keepdims=True)
            row_dot = jnp.sum(lift * dots[:, cols], axis=0, keepdims=True) * inverse_total
            scales[:, cols] = lift * inverse_total

            def second(j):
                base = pl.multiple_of(j * keys, LANES)
                rng = pl.ds(base, keys)
                for b in range(per):
                    here = pl.ds(base + b * LANES, LANES)
                    row = pl.ds(j * per + b, 1)
                    probs = weights_buf[here, cols] * scales[row, cols]
                    grad_probs = grad_buf[here, cols]
                    low_buf[here, cols] = probs.astype(bf16)
                    mixed_buf[here, cols] = (probs * grad_probs).astype(bf16)
                    scores_grad_buf[here, cols] = (probs * (grad_probs - row_dot)).astype(bf16)
                dv_acc[rng, :] += jnp.dot(low_buf[rng, cols], grads, preferred_element_type=f32)
                dk_acc[rng, :] += jnp.dot(
                    scores_grad_buf[rng, cols], qn, preferred_element_type=f32
                )

            over_keys(second)
            weighted_grad = jnp.dot(kn_t[...], mixed_buf[:, cols], preferred_element_type=f32)
            weighted_keys = jnp.dot(kn_t[...], low_buf[:, cols], preferred_element_type=f32)
            grad_q = ((weighted_grad - row_dot * weighted_keys) * factor).T
            result, text_sum, image_sum = finish(grad_q, unit, inverse, text, gains)
            dq_buf[at, :] = result
            gain_mine[0:1, :] += text_sum
            gain_mine[1:2, :] += image_sum

        def send_range(begin, end, flip):
            @pl.loop(begin, end)
            def _(k):
                send_back(0, real(jnp.where(flip, n - 1 - k, k), n))

        def place(i):
            down = jnp.logical_and(turn, i >= half)
            return down, jnp.where(down, i - half, i)

        def send_done(i):
            down, t = place(i)
            send_range((CHUNK * t) // rows, (CHUNK * (t + 1)) // rows, down)

        @pl.loop(0, full)
        def _(i):
            down, t = place(i)
            need = (CHUNK * (t + 1) - 1) // rows + 1
            had = jnp.where(t == 0, 0, (CHUNK * t - 1) // rows + 1)
            need = jnp.where(down, jnp.minimum(need, n - half_need), need)

            @pl.loop(had, need)
            def _(k):
                src = real(jnp.where(down, n - 1 - k, k), n)
                wait_in(2, src)
                wait_in(3, src)

            @pl.when(i == full - 1)
            def _():
                @pl.loop(0, full - 1)
                def _(k):
                    send_done(k)

            begin = jnp.where(down, total - CHUNK * (t + 1), CHUNK * t)
            attend(jnp.where(low, begin, total - CHUNK - begin), CHUNK)
            @pl.when(i == full - 1)
            def _():
                send_done(i)

        if tail:
            had_all = (CHUNK * full - 1) // rows + 1
            left_had = (CHUNK * (full - half) - 1) // rows + 1
            seen = jnp.where(turn, jnp.minimum(half_need + left_had, n), had_all)

            @pl.loop(seen, n)
            def _(k):
                k = jnp.where(turn, half_need + k - seen, k)
                wait_in(2, real(k, n))
                wait_in(3, real(k, n))

            begin = jnp.where(turn, CHUNK * half, CHUNK * full)
            attend(jnp.where(low, begin, total - tail - begin), tail)
        send_range(
            jnp.where(turn, half_done, (CHUNK * full) // rows),
            jnp.where(turn, n - rest_done, n),
            False,
        )

        @pl.loop(0, tiles)
        def _(c):
            at = pl.ds(pl.multiple_of(c * LANES, LANES), LANES)
            text, gains = gains_at(kg_ref, c * LANES, LANES)
            unit, inverse = unit_of(k_all[at, :])
            result, text_sum, image_sum = finish(
                dk_acc[at, :] * factor, unit, inverse, text, gains
            )
            dk_buf[at, :] = result
            gain_mine[2:3, :] += text_sum
            gain_mine[3:4, :] += image_sum

        @pl.loop(1, n)
        def _(s):
            gain_copy(partner(me, s, n)).start()

        pltpu.make_async_copy(gain_mine, gain_heads.at[mine], g1_recv.at[mine]).start()

        dv_buf[...] = dv_acc[...].astype(bf16)

        def far_first(s):
            return jnp.where(low, n - 1 - s, s)

        @pl.loop(0, n)
        def _(s):
            send_back(2, far_first(s))

        @pl.loop(0, n)
        def _(s):
            send_back(1, far_first(s))

    for h in range(heads):
        pltpu.make_async_copy(gain_mine, gain_heads.at[h], g1_recv.at[h]).wait()
    group = gain_heads[0]
    for h in range(1, heads):
        group = group + gain_heads[h]
    gain_group[...] = group
    for s in range(1, n_uly):
        uly_copy(s).start()
    gain_uly[uly] = group
    for s in range(1, n_uly):
        src = (uly + s) % n_uly
        pltpu.make_async_copy(gain_group, gain_uly.at[src], g2_recv.at[src]).wait()
    summed = gain_uly[0]
    for u in range(1, n_uly):
        summed = summed + gain_uly[u]
    q_gain_out[...] = summed[0:2, :]
    k_gain_out[...] = summed[2:4, :]

    for s in range(1, n_uly):
        uly_copy(s).wait_send()

    for a in range(3):
        for h in range(heads):
            pltpu.make_async_copy(
                backs[a].at[block(0)], outs[a].at[h], back_recv.at[a, h]
            ).wait()

    @pl.when(i_own)
    def _():
        @pl.loop(1, n)
        def _(s):
            gain_copy(partner(me, s, n)).wait_send()

        @pl.loop(1, n)
        def _(s):
            dev = partner(me, s, n)
            for a in range(3):
                back_copy(a, dev).wait_send()

    @pl.loop(1, n)
    def _(s):
        dev = partner(me, s, n)

        @pl.when(owns(dev))
        def _():
            for a in range(4):
                in_copy(a, s, head_of(dev), dev).wait_send()


def store(*refs):
    count = len(refs) // 2
    sems = refs[-1]
    copies = [
        pltpu.make_async_copy(refs[i], refs[count + i], sems.at[i]) for i in range(count)
    ]
    for copy in copies:
        copy.start()
    for copy in copies:
        copy.wait()


def solution(mesh):
    n, n_uly = mesh.shape["blk"], mesh.shape["uly"]

    def local(q_raw, k_raw, values, out_grad, q_gain, k_gain):
        rows, heads, width = q_raw.shape
        total = n * rows
        vmem = pl.BlockSpec(memory_space=pltpu.VMEM)
        first = [jnp.transpose(x, (1, 0, 2)) for x in (k_raw, values, q_raw, out_grad)]
        out_block = jax.ShapeDtypeStruct((heads, rows, width), bf16)
        hbm = pl.BlockSpec(memory_space=pltpu.HBM)
        gain_block = jax.ShapeDtypeStruct((2, width), f32)
        shapes = (out_block,) * 3 + (gain_block,) * 2
        results = pl.pallas_call(
            functools.partial(kernel, n, n_uly, heads, rows),
            out_shape=shapes,
            in_specs=[hbm] * 6,
            out_specs=(vmem,) * 5,
            scratch_shapes=[pltpu.VMEM((heads, rows, width), bf16)] * 4
            + [pltpu.VMEM((total, width), bf16)] * 5
            + [pltpu.VMEM((width, total), bf16)]
            + [pltpu.VMEM((total, width), f32)] * 2
            + [pltpu.VMEM((total, width), bf16)] * 3
            + [pltpu.VMEM((total, CHUNK), f32)] * 2
            + [pltpu.VMEM((total, CHUNK), bf16)] * 3
            + [pltpu.VMEM((total // LANES, CHUNK), f32)] * 4
            + [
                pltpu.VMEM((2, width), f32),
                pltpu.VMEM((2, width), f32),
                pltpu.VMEM((4, width), f32),
                pltpu.VMEM((heads, 4, width), f32),
                pltpu.VMEM((4, width), f32),
                pltpu.VMEM((n_uly, 4, width), f32),
                pltpu.SemaphoreType.DMA((6,)),
                pltpu.SemaphoreType.DMA((4, n)),
                pltpu.SemaphoreType.DMA((4, n)),
                pltpu.SemaphoreType.DMA((3, n)),
                pltpu.SemaphoreType.DMA((3, heads)),
                pltpu.SemaphoreType.DMA((n,)),
                pltpu.SemaphoreType.DMA((heads,)),
                pltpu.SemaphoreType.DMA((n_uly,)),
                pltpu.SemaphoreType.DMA((n_uly,)),
            ],
            compiler_params=pltpu.CompilerParams(
                collective_id=0, has_side_effects=True, vmem_limit_bytes=67043328
            ),
        )(*first, q_gain, k_gain)
        dq, dk, dv, q_total, k_total = pl.pallas_call(
            store,
            out_shape=shapes,
            in_specs=[vmem] * 5,
            out_specs=(hbm,) * 5,
            scratch_shapes=[pltpu.SemaphoreType.DMA((5,))],
        )(*results)
        back = [jnp.transpose(x, (1, 0, 2)) for x in (dq, dk, dv)]
        return (*back, q_total, k_total)

    placed = (P("blk", "uly", None),) * 4 + (P(), P())
    return jax.shard_map(
        local,
        mesh=mesh,
        in_specs=placed,
        out_specs=(P("blk", "uly", None),) * 3 + (P(), P()),
        check_vma=False,
    )
```

```python
import functools
import math

import jax
import jax.numpy as jnp
from jax import lax
from jax.experimental import pallas as pl
from jax.experimental.pallas import tpu as pltpu
from jax.sharding import PartitionSpec as P

TXT = 512
EPS = 1e-06
LANES = 128
CHUNK = 256
KEYS = 1152
KERNEL_VMEM = 48 * 2**20
STORE_VMEM = 2**20
MESH = pl.DeviceIdType.MESH
f32, bf16 = jnp.float32, jnp.bfloat16


def partner(me, step, n):
    if n & (n - 1):
        return (me + step) % n
    out, bit = 0, 1
    while bit < n:
        out = out + ((me // bit + step // bit) % 2) * bit
        bit *= 2
    return out


def kernel(
    n, n_uly, heads, rows,
    k_hbm, v_hbm, q_hbm, g_hbm, qg_hbm, kg_hbm,
    dq_out, dk_out, dv_out, q_gain_out, k_gain_out,
    k_in, v_in, q_in, g_in,
    k_all, v_all, q_all, g_all, kn, kn_t, dk_acc, dv_acc, dq_buf, dk_buf, dv_buf,
    weights_buf, grad_buf, low_buf, mixed_buf, scores_grad_buf, peaks, sums, dots, scales,
    qg_ref, kg_ref, gain_mine, gain_heads, gain_group, gain_uly,
    staged, in_send, in_recv, back_send, back_recv, g1_send, g1_recv, g2_send, g2_recv,
):
    me = lax.axis_index("blk")
    uly = lax.axis_index("uly")
    total = n * rows
    full = total // CHUNK
    tail = total - full * CHUNK
    tiles = total // LANES
    width = k_in.shape[2]
    factor = 1.0 / math.sqrt(width)
    factor2 = factor * math.log2(math.e)
    keys = max(d for d in range(LANES, min(total, KEYS) + 1, LANES) if total % d == 0)
    phase = (uly % 2) * (heads % n)

    def head_of(dev):
        return (heads * dev + phase) // n

    def owns(dev):
        return (heads * dev + phase) % n + heads >= n

    def owner(h):
        return ((h + 1) * n - phase + heads - 1) // heads - 1

    mine = head_of(me)
    i_own = owns(me)

    sources = (k_hbm, v_hbm, q_hbm, g_hbm)
    ins = (k_in, v_in, q_in, g_in)
    alls = (k_all, v_all, q_all, g_all)
    backs = (dq_buf, dk_buf, dv_buf)
    outs = (dq_out, dk_out, dv_out)

    def block(dev):
        return pl.ds(pl.multiple_of(dev * rows, 16), rows)

    def stage(a):
        return pltpu.make_async_copy(sources[a], ins[a], staged.at[a])

    gain_stages = (
        pltpu.make_async_copy(qg_hbm, qg_ref, staged.at[4]),
        pltpu.make_async_copy(kg_hbm, kg_ref, staged.at[5]),
    )

    barrier = pltpu.get_barrier_semaphore()
    for s in range(1, n):
        pl.semaphore_signal(
            barrier, inc=1, device_id={"blk": partner(me, s, n)}, device_id_type=MESH
        )
    for s in range(1, n_uly):
        pl.semaphore_signal(
            barrier, inc=1, device_id={"uly": (uly + s) % n_uly}, device_id_type=MESH
        )
    for a in range(4):
        stage(a).start()
    for copy in gain_stages:
        copy.start()
    pl.semaphore_wait(barrier, n - 1 + n_uly - 1)

    def in_copy(a, s, h, dev):
        return pltpu.make_async_remote_copy(
            src_ref=ins[a].at[h], dst_ref=alls[a].at[block(me)],
            send_sem=in_send.at[a, s], recv_sem=in_recv.at[a, me],
            device_id={"blk": dev}, device_id_type=MESH,
        )

    def send_in(a, s):
        dev = partner(me, s, n)

        @pl.when(owns(dev))
        def _():
            in_copy(a, s, head_of(dev), dev).start()

    def keep_in(a):
        @pl.when(i_own)
        def _():
            pltpu.make_async_copy(
                ins[a].at[mine], alls[a].at[block(me)], in_recv.at[a, me]
            ).start()

    def wait_in(a, src):
        pltpu.make_async_copy(ins[a].at[0], alls[a].at[block(src)], in_recv.at[a, src]).wait()

    for a in (0, 1):
        stage(a).wait()
        for s in range(n - 1, 0, -1):
            send_in(a, s)
    for a in (2, 3):
        stage(a).wait()
    for copy in gain_stages:
        copy.wait()
    for a in range(4):
        keep_in(a)
    for s in range(1, n):
        for a in (2, 3):
            send_in(a, s)

    def back_copy(a, dev):
        return pltpu.make_async_remote_copy(
            src_ref=backs[a].at[block(dev)], dst_ref=outs[a].at[mine],
            send_sem=back_send.at[a, dev], recv_sem=back_recv.at[a, mine],
            device_id={"blk": dev}, device_id_type=MESH,
        )

    def send_back(a, dev):
        @pl.when(dev != me)
        def _():
            back_copy(a, dev).start()

        @pl.when(dev == me)
        def _():
            pltpu.make_async_copy(
                backs[a].at[block(dev)], outs[a].at[mine], back_recv.at[a, mine]
            ).start()

    def gain_copy(dev):
        return pltpu.make_async_remote_copy(
            src_ref=gain_mine, dst_ref=gain_heads.at[mine],
            send_sem=g1_send.at[dev], recv_sem=g1_recv.at[mine],
            device_id={"blk": dev}, device_id_type=MESH,
        )

    def uly_copy(s):
        return pltpu.make_async_remote_copy(
            src_ref=gain_group, dst_ref=gain_uly.at[uly],
            send_sem=g2_send.at[s], recv_sem=g2_recv.at[uly],
            device_id={"uly": (uly + s) % n_uly}, device_id_type=MESH,
        )

    def gains_at(gain_ref, base, size):
        position = base + lax.broadcasted_iota(jnp.int32, (size, width), 0)
        text = position < TXT
        return text, jnp.where(text, gain_ref[0:1, :], gain_ref[1:2, :])

    def unit_of(raw):
        wide = raw.astype(f32)
        inverse = lax.rsqrt(jnp.mean(wide * wide, axis=-1, keepdims=True) + EPS)
        return wide * inverse, inverse

    def finish(grad, unit, inverse, text, gains):
        part = grad * unit
        scaled = grad * gains
        text_sum = jnp.sum(jnp.where(text, part, 0.0), axis=0, keepdims=True)
        image_sum = jnp.sum(jnp.where(text, 0.0, part), axis=0, keepdims=True)
        result = (scaled - unit * jnp.mean(scaled * unit, axis=-1, keepdims=True)) * inverse
        return result.astype(bf16), text_sum, image_sum

    @pl.when(i_own)
    def _():
        low = me < n // 2
        turn = jnp.where(low, me, n - 1 - me) >= n // 4
        half = full // 2
        half_need = (CHUNK * half - 1) // rows + 1
        half_done = (CHUNK * half) // rows
        rest_done = (CHUNK * (full - half)) // rows
        nt = (((1,), (1,)), ((), ()))

        def real(i, count):
            return jnp.where(low, i, count - 1 - i)

        gain_mine[...] = jnp.zeros_like(gain_mine)
        dk_acc[...] = jnp.zeros_like(dk_acc)
        dv_acc[...] = jnp.zeros_like(dv_acc)

        @pl.loop(0, n)
        def _(src):
            wait_in(0, src)

        @pl.loop(0, tiles)
        def _(c):
            at = pl.ds(pl.multiple_of(c * LANES, LANES), LANES)
            text, gains = gains_at(kg_ref, c * LANES, LANES)
            unit, _inverse = unit_of(k_all[at, :])
            normed = unit * gains
            kn[at, :] = normed.astype(bf16)
            kn_t[:, at] = normed.T.astype(bf16)

        @pl.loop(0, n)
        def _(src):
            wait_in(1, src)

        def over_keys(body):
            if keys == total:
                body(0)
            else:
                @pl.loop(0, total // keys)
                def _(j):
                    body(j)

        def attend(start, size):
            start = pl.multiple_of(start, LANES)
            at = pl.ds(start, size)
            text, gains = gains_at(qg_ref, start, size)
            unit, inverse = unit_of(q_all[at, :])
            qn = (unit * gains).astype(bf16)
            grads = g_all[at, :]
            cols = pl.ds(0, size)
            per = keys // LANES

            def first(j):
                base = pl.multiple_of(j * keys, LANES)
                rng = pl.ds(base, keys)
                scores = lax.dot_general(kn[rng, :], qn, nt, preferred_element_type=f32)
                grad_probs = lax.dot_general(v_all[rng, :], grads, nt, preferred_element_type=f32)
                for b in range(per):
                    part = slice(b * LANES, (b + 1) * LANES)
                    here = pl.ds(base + b * LANES, LANES)
                    row = pl.ds(j * per + b, 1)
                    peak = jnp.max(scores[part], axis=0, keepdims=True)
                    weights = jnp.exp2((scores[part] - peak) * factor2)
                    peaks[row, cols] = peak
                    sums[row, cols] = jnp.sum(weights, axis=0, keepdims=True)
                    dots[row, cols] = jnp.sum(weights * grad_probs[part], axis=0, keepdims=True)
                    weights_buf[here, cols] = weights
                    grad_buf[here, cols] = grad_probs[part]

            over_keys(first)
            peak_all = peaks[:, cols]
            lift = jnp.exp2((peak_all - jnp.max(peak_all, axis=0, keepdims=True)) * factor2)
            inverse_total = 1.0 / jnp.sum(lift * sums[:, cols], axis=0, keepdims=True)
            row_dot = jnp.sum(lift * dots[:, cols], axis=0, keepdims=True) * inverse_total
            scales[:, cols] = lift * inverse_total

            def second(j):
                base = pl.multiple_of(j * keys, LANES)
                rng = pl.ds(base, keys)
                for b in range(per):
                    here = pl.ds(base + b * LANES, LANES)
                    row = pl.ds(j * per + b, 1)
                    probs = weights_buf[here, cols] * scales[row, cols]
                    grad_probs = grad_buf[here, cols]
                    low_buf[here, cols] = probs.astype(bf16)
                    mixed_buf[here, cols] = (probs * grad_probs).astype(bf16)
                    scores_grad_buf[here, cols] = (probs * (grad_probs - row_dot)).astype(bf16)
                dv_acc[rng, :] += jnp.dot(low_buf[rng, cols], grads, preferred_element_type=f32)
                dk_acc[rng, :] += jnp.dot(
                    scores_grad_buf[rng, cols], qn, preferred_element_type=f32
                )

            over_keys(second)
            weighted_grad = jnp.dot(kn_t[...], mixed_buf[:, cols], preferred_element_type=f32)
            weighted_keys = jnp.dot(kn_t[...], low_buf[:, cols], preferred_element_type=f32)
            grad_q = ((weighted_grad - row_dot * weighted_keys) * factor).T
            result, text_sum, image_sum = finish(grad_q, unit, inverse, text, gains)
            dq_buf[at, :] = result
            gain_mine[0:1, :] += text_sum
            gain_mine[1:2, :] += image_sum

        def send_range(begin, end, flip):
            @pl.loop(begin, end)
            def _(k):
                send_back(0, real(jnp.where(flip, n - 1 - k, k), n))

        def place(i):
            down = jnp.logical_and(turn, i >= half)
            return down, jnp.where(down, i - half, i)

        def send_done(i):
            down, t = place(i)
            send_range((CHUNK * t) // rows, (CHUNK * (t + 1)) // rows, down)

        @pl.loop(0, full)
        def _(i):
            down, t = place(i)
            need = (CHUNK * (t + 1) - 1) // rows + 1
            had = jnp.where(t == 0, 0, (CHUNK * t - 1) // rows + 1)
            need = jnp.where(down, jnp.minimum(need, n - half_need), need)

            @pl.loop(had, need)
            def _(k):
                src = real(jnp.where(down, n - 1 - k, k), n)
                wait_in(2, src)
                wait_in(3, src)

            @pl.when(i == full - 1)
            def _():
                @pl.loop(0, full - 1)
                def _(k):
                    send_done(k)

            begin = jnp.where(down, total - CHUNK * (t + 1), CHUNK * t)
            attend(jnp.where(low, begin, total - CHUNK - begin), CHUNK)
            @pl.when(i == full - 1)
            def _():
                send_done(i)

        if tail:
            had_all = (CHUNK * full - 1) // rows + 1
            left_had = (CHUNK * (full - half) - 1) // rows + 1
            seen = jnp.where(turn, jnp.minimum(half_need + left_had, n), had_all)

            @pl.loop(seen, n)
            def _(k):
                k = jnp.where(turn, half_need + k - seen, k)
                wait_in(2, real(k, n))
                wait_in(3, real(k, n))

            begin = jnp.where(turn, CHUNK * half, CHUNK * full)
            attend(jnp.where(low, begin, total - tail - begin), tail)
        send_range(
            jnp.where(turn, half_done, (CHUNK * full) // rows),
            jnp.where(turn, n - rest_done, n),
            False,
        )

        @pl.loop(0, tiles)
        def _(c):
            at = pl.ds(pl.multiple_of(c * LANES, LANES), LANES)
            text, gains = gains_at(kg_ref, c * LANES, LANES)
            unit, inverse = unit_of(k_all[at, :])
            result, text_sum, image_sum = finish(
                dk_acc[at, :] * factor, unit, inverse, text, gains
            )
            dk_buf[at, :] = result
            gain_mine[2:3, :] += text_sum
            gain_mine[3:4, :] += image_sum

        @pl.loop(1, n)
        def _(s):
            gain_copy(partner(me, s, n)).start()

        pltpu.make_async_copy(gain_mine, gain_heads.at[mine], g1_recv.at[mine]).start()

        dv_buf[...] = dv_acc[...].astype(bf16)

        def far_first(s):
            return jnp.where(low, n - 1 - s, s)

        @pl.loop(0, n)
        def _(s):
            send_back(2, far_first(s))

        @pl.loop(0, n)
        def _(s):
            send_back(1, far_first(s))

    for h in range(heads):
        pltpu.make_async_copy(gain_mine, gain_heads.at[h], g1_recv.at[h]).wait()
    group = gain_heads[0]
    for h in range(1, heads):
        group = group + gain_heads[h]
    gain_group[...] = group
    for s in range(1, n_uly):
        uly_copy(s).start()
    gain_uly[uly] = group
    for s in range(1, n_uly):
        src = (uly + s) % n_uly
        pltpu.make_async_copy(gain_group, gain_uly.at[src], g2_recv.at[src]).wait()
    summed = gain_uly[0]
    for u in range(1, n_uly):
        summed = summed + gain_uly[u]
    q_gain_out[...] = summed[0:2, :]
    k_gain_out[...] = summed[2:4, :]

    for s in range(1, n_uly):
        uly_copy(s).wait_send()

    for a in range(3):
        for h in range(heads):
            pltpu.make_async_copy(
                backs[a].at[block(0)], outs[a].at[h], back_recv.at[a, h]
            ).wait()

    @pl.when(i_own)
    def _():
        @pl.loop(1, n)
        def _(s):
            gain_copy(partner(me, s, n)).wait_send()

        @pl.loop(1, n)
        def _(s):
            dev = partner(me, s, n)
            for a in range(3):
                back_copy(a, dev).wait_send()

    @pl.loop(1, n)
    def _(s):
        dev = partner(me, s, n)

        @pl.when(owns(dev))
        def _():
            for a in range(4):
                in_copy(a, s, head_of(dev), dev).wait_send()


def store(*refs):
    count = len(refs) // 2
    sems = refs[-1]
    copies = [
        pltpu.make_async_copy(refs[i], refs[count + i], sems.at[i]) for i in range(count)
    ]
    for copy in copies:
        copy.start()
    for copy in copies:
        copy.wait()


def solution(mesh):
    n, n_uly = mesh.shape["blk"], mesh.shape["uly"]

    def local(q_raw, k_raw, values, out_grad, q_gain, k_gain):
        rows, heads, width = q_raw.shape
        total = n * rows
        vmem = pl.BlockSpec(memory_space=pltpu.VMEM)
        first = [jnp.transpose(x, (1, 0, 2)) for x in (k_raw, values, q_raw, out_grad)]
        out_block = jax.ShapeDtypeStruct((heads, rows, width), bf16)
        hbm = pl.BlockSpec(memory_space=pltpu.HBM)
        gain_block = jax.ShapeDtypeStruct((2, width), f32)
        shapes = (out_block,) * 3 + (gain_block,) * 2
        held = tuple(pltpu.VMEM(x.shape, x.dtype) for x in shapes)
        results = pl.pallas_call(
            functools.partial(kernel, n, n_uly, heads, rows),
            out_shape=held,
            in_specs=[hbm] * 6,
            out_specs=(vmem,) * 5,
            scratch_shapes=[pltpu.VMEM((heads, rows, width), bf16)] * 4
            + [pltpu.VMEM((total, width), bf16)] * 5
            + [pltpu.VMEM((width, total), bf16)]
            + [pltpu.VMEM((total, width), f32)] * 2
            + [pltpu.VMEM((total, width), bf16)] * 3
            + [pltpu.VMEM((total, CHUNK), f32)] * 2
            + [pltpu.VMEM((total, CHUNK), bf16)] * 3
            + [pltpu.VMEM((total // LANES, CHUNK), f32)] * 4
            + [
                pltpu.VMEM((2, width), f32),
                pltpu.VMEM((2, width), f32),
                pltpu.VMEM((4, width), f32),
                pltpu.VMEM((heads, 4, width), f32),
                pltpu.VMEM((4, width), f32),
                pltpu.VMEM((n_uly, 4, width), f32),
                pltpu.SemaphoreType.DMA((6,)),
                pltpu.SemaphoreType.DMA((4, n)),
                pltpu.SemaphoreType.DMA((4, n)),
                pltpu.SemaphoreType.DMA((3, n)),
                pltpu.SemaphoreType.DMA((3, heads)),
                pltpu.SemaphoreType.DMA((n,)),
                pltpu.SemaphoreType.DMA((heads,)),
                pltpu.SemaphoreType.DMA((n_uly,)),
                pltpu.SemaphoreType.DMA((n_uly,)),
            ],
            compiler_params=pltpu.CompilerParams(
                collective_id=0, has_side_effects=True, vmem_limit_bytes=KERNEL_VMEM
            ),
        )(*[pltpu.with_memory_space_constraint(x, pltpu.HBM) for x in (*first, q_gain, k_gain)])
        dq, dk, dv, q_total, k_total = pl.pallas_call(
            store,
            out_shape=shapes,
            in_specs=[vmem] * 5,
            out_specs=(hbm,) * 5,
            scratch_shapes=[pltpu.SemaphoreType.DMA((5,))],
            compiler_params=pltpu.CompilerParams(vmem_limit_bytes=STORE_VMEM),
        )(*results)
        back = [jnp.transpose(x, (1, 0, 2)) for x in (dq, dk, dv)]
        return (*back, q_total, k_total)

    placed = (P("blk", "uly", None),) * 4 + (P(), P())
    return jax.shard_map(
        local,
        mesh=mesh,
        in_specs=placed,
        out_specs=(P("blk", "uly", None),) * 3 + (P(), P()),
        check_vma=False,
    )
```

```python
import functools
import math

import jax
import jax.numpy as jnp
from jax import lax
from jax.experimental import pallas as pl
from jax.experimental.pallas import tpu as pltpu
from jax.sharding import PartitionSpec as P

TXT = 512
EPS = 1e-06
LANES = 128
CHUNK = 256
KEYS = 1152
KERNEL_VMEM = 48 * 2**20
STORE_VMEM = 2**20
MESH = pl.DeviceIdType.MESH
f32, bf16 = jnp.float32, jnp.bfloat16


def partner(me, step, n):
    if n & (n - 1):
        return (me + step) % n
    out, bit = 0, 1
    while bit < n:
        out = out + ((me // bit + step // bit) % 2) * bit
        bit *= 2
    return out


def kernel(
    n, n_uly, heads, rows,
    k_hbm, v_hbm, q_hbm, g_hbm, qg_hbm, kg_hbm,
    dq_out, dk_out, dv_out, q_gain_out, k_gain_out,
    k_in, v_in, q_in, g_in,
    k_all, v_all, q_all, g_all, kn, kn_t, dk_acc, dv_acc, dq_buf, dk_buf, dv_buf,
    weights_buf, grad_buf, low_buf, mixed_buf, scores_grad_buf, peaks, sums, dots, scales,
    qg_ref, kg_ref, gain_mine, gain_heads, gain_group, gain_uly,
    staged, in_send, in_recv, back_send, back_recv, g1_send, g1_recv, g2_send, g2_recv, entered,
):
    me = lax.axis_index("blk")
    uly = lax.axis_index("uly")
    total = n * rows
    full = total // CHUNK
    tail = total - full * CHUNK
    tiles = total // LANES
    width = k_in.shape[2]
    factor = 1.0 / math.sqrt(width)
    factor2 = factor * math.log2(math.e)
    keys = max(d for d in range(LANES, min(total, KEYS) + 1, LANES) if total % d == 0)
    phase = (uly % 2) * (heads % n)

    def head_of(dev):
        return (heads * dev + phase) // n

    def owns(dev):
        return (heads * dev + phase) % n + heads >= n

    def owner(h):
        return ((h + 1) * n - phase + heads - 1) // heads - 1

    mine = head_of(me)
    i_own = owns(me)

    sources = (k_hbm, v_hbm, q_hbm, g_hbm)
    ins = (k_in, v_in, q_in, g_in)
    alls = (k_all, v_all, q_all, g_all)
    backs = (dq_buf, dk_buf, dv_buf)
    outs = (dq_out, dk_out, dv_out)

    def block(dev):
        return pl.ds(pl.multiple_of(dev * rows, 16), rows)

    def stage(a):
        return pltpu.make_async_copy(sources[a], ins[a], staged.at[a])

    gain_stages = (
        pltpu.make_async_copy(qg_hbm, qg_ref, staged.at[4]),
        pltpu.make_async_copy(kg_hbm, kg_ref, staged.at[5]),
    )

    quarter = n // 4

    def inner(dev):
        return jnp.logical_and(dev >= quarter, dev < n - quarter)

    i_inner = inner(me)
    pair = jnp.where((me // quarter) % 2 == 0, me + quarter, me - quarter)
    barrier = pltpu.get_barrier_semaphore()
    for s in range(1, n_uly):
        pl.semaphore_signal(
            barrier, inc=1, device_id={"uly": (uly + s) % n_uly}, device_id_type=MESH
        )

    @pl.when(i_inner)
    def _():
        @pl.loop(quarter, n - quarter)
        def _(dev):
            @pl.when(dev != me)
            def _():
                pl.semaphore_signal(barrier, inc=1, device_id={"blk": dev}, device_id_type=MESH)

    for a in range(4):
        stage(a).start()
    for copy in gain_stages:
        copy.start()

    @pl.when(i_inner)
    def _():
        pl.semaphore_wait(barrier, n - 2 * quarter - 1 + n_uly - 1)
        pl.semaphore_signal(barrier, inc=1, device_id={"blk": pair}, device_id_type=MESH)

    @pl.when(jnp.logical_not(i_inner))
    def _():
        pl.semaphore_wait(barrier, 1 + n_uly - 1)

        @pl.loop(quarter, n - quarter)
        def _(dev):
            pl.semaphore_signal(entered, inc=1, device_id={"blk": dev}, device_id_type=MESH)

    def meet():
        @pl.when(i_inner)
        def _():
            pl.semaphore_wait(entered, 2 * quarter)
            pl.semaphore_signal(entered, inc=1, device_id={"blk": pair}, device_id_type=MESH)

        @pl.when(jnp.logical_not(i_inner))
        def _():
            pl.semaphore_wait(entered, 1)

    def in_copy(a, s, h, dev):
        return pltpu.make_async_remote_copy(
            src_ref=ins[a].at[h], dst_ref=alls[a].at[block(me)],
            send_sem=in_send.at[a, s], recv_sem=in_recv.at[a, me],
            device_id={"blk": dev}, device_id_type=MESH,
        )

    def send_in(a, s, near=None):
        dev = partner(me, s, n)
        wanted = owns(dev)
        if near is not None:
            wanted = jnp.logical_and(wanted, inner(dev) == near)

        @pl.when(wanted)
        def _():
            in_copy(a, s, head_of(dev), dev).start()

    def keep_in(a):
        @pl.when(i_own)
        def _():
            pltpu.make_async_copy(
                ins[a].at[mine], alls[a].at[block(me)], in_recv.at[a, me]
            ).start()

    def wait_in(a, src):
        pltpu.make_async_copy(ins[a].at[0], alls[a].at[block(src)], in_recv.at[a, src]).wait()

    for first in (True, False):
        for a in (0, 1):
            if first:
                stage(a).wait()
            for s in range(n - 1, 0, -1):
                send_in(a, s, first)
        if first:
            meet()
    for a in (2, 3):
        stage(a).wait()
    for copy in gain_stages:
        copy.wait()
    for a in range(4):
        keep_in(a)
    for s in range(1, n):
        for a in (2, 3):
            send_in(a, s)

    def back_copy(a, dev):
        return pltpu.make_async_remote_copy(
            src_ref=backs[a].at[block(dev)], dst_ref=outs[a].at[mine],
            send_sem=back_send.at[a, dev], recv_sem=back_recv.at[a, mine],
            device_id={"blk": dev}, device_id_type=MESH,
        )

    def send_back(a, dev):
        @pl.when(dev != me)
        def _():
            back_copy(a, dev).start()

        @pl.when(dev == me)
        def _():
            pltpu.make_async_copy(
                backs[a].at[block(dev)], outs[a].at[mine], back_recv.at[a, mine]
            ).start()

    def gain_copy(dev):
        return pltpu.make_async_remote_copy(
            src_ref=gain_mine, dst_ref=gain_heads.at[mine],
            send_sem=g1_send.at[dev], recv_sem=g1_recv.at[mine],
            device_id={"blk": dev}, device_id_type=MESH,
        )

    def uly_copy(s):
        return pltpu.make_async_remote_copy(
            src_ref=gain_group, dst_ref=gain_uly.at[uly],
            send_sem=g2_send.at[s], recv_sem=g2_recv.at[uly],
            device_id={"uly": (uly + s) % n_uly}, device_id_type=MESH,
        )

    def gains_at(gain_ref, base, size):
        position = base + lax.broadcasted_iota(jnp.int32, (size, width), 0)
        text = position < TXT
        return text, jnp.where(text, gain_ref[0:1, :], gain_ref[1:2, :])

    def unit_of(raw):
        wide = raw.astype(f32)
        inverse = lax.rsqrt(jnp.mean(wide * wide, axis=-1, keepdims=True) + EPS)
        return wide * inverse, inverse

    def finish(grad, unit, inverse, text, gains):
        part = grad * unit
        scaled = grad * gains
        text_sum = jnp.sum(jnp.where(text, part, 0.0), axis=0, keepdims=True)
        image_sum = jnp.sum(jnp.where(text, 0.0, part), axis=0, keepdims=True)
        result = (scaled - unit * jnp.mean(scaled * unit, axis=-1, keepdims=True)) * inverse
        return result.astype(bf16), text_sum, image_sum

    @pl.when(i_own)
    def _():
        low = me < n // 2
        turn = jnp.where(low, me, n - 1 - me) >= n // 4
        half = full // 2
        half_need = (CHUNK * half - 1) // rows + 1
        half_done = (CHUNK * half) // rows
        rest_done = (CHUNK * (full - half)) // rows
        nt = (((1,), (1,)), ((), ()))

        def real(i, count):
            return jnp.where(low, i, count - 1 - i)

        gain_mine[...] = jnp.zeros_like(gain_mine)
        dk_acc[...] = jnp.zeros_like(dk_acc)
        dv_acc[...] = jnp.zeros_like(dv_acc)

        @pl.loop(0, n)
        def _(src):
            wait_in(0, src)

        @pl.loop(0, tiles)
        def _(c):
            at = pl.ds(pl.multiple_of(c * LANES, LANES), LANES)
            text, gains = gains_at(kg_ref, c * LANES, LANES)
            unit, _inverse = unit_of(k_all[at, :])
            normed = unit * gains
            kn[at, :] = normed.astype(bf16)
            kn_t[:, at] = normed.T.astype(bf16)

        @pl.loop(0, n)
        def _(src):
            wait_in(1, src)

        def over_keys(body):
            if keys == total:
                body(0)
            else:
                @pl.loop(0, total // keys)
                def _(j):
                    body(j)

        def attend(start, size):
            start = pl.multiple_of(start, LANES)
            at = pl.ds(start, size)
            text, gains = gains_at(qg_ref, start, size)
            unit, inverse = unit_of(q_all[at, :])
            qn = (unit * gains).astype(bf16)
            grads = g_all[at, :]
            cols = pl.ds(0, size)
            per = keys // LANES

            def first(j):
                base = pl.multiple_of(j * keys, LANES)
                rng = pl.ds(base, keys)
                scores = lax.dot_general(kn[rng, :], qn, nt, preferred_element_type=f32)
                grad_probs = lax.dot_general(v_all[rng, :], grads, nt, preferred_element_type=f32)
                for b in range(per):
                    part = slice(b * LANES, (b + 1) * LANES)
                    here = pl.ds(base + b * LANES, LANES)
                    row = pl.ds(j * per + b, 1)
                    peak = jnp.max(scores[part], axis=0, keepdims=True)
                    weights = jnp.exp2((scores[part] - peak) * factor2)
                    peaks[row, cols] = peak
                    sums[row, cols] = jnp.sum(weights, axis=0, keepdims=True)
                    dots[row, cols] = jnp.sum(weights * grad_probs[part], axis=0, keepdims=True)
                    weights_buf[here, cols] = weights
                    grad_buf[here, cols] = grad_probs[part]

            over_keys(first)
            peak_all = peaks[:, cols]
            lift = jnp.exp2((peak_all - jnp.max(peak_all, axis=0, keepdims=True)) * factor2)
            inverse_total = 1.0 / jnp.sum(lift * sums[:, cols], axis=0, keepdims=True)
            row_dot = jnp.sum(lift * dots[:, cols], axis=0, keepdims=True) * inverse_total
            scales[:, cols] = lift * inverse_total

            def second(j):
                base = pl.multiple_of(j * keys, LANES)
                rng = pl.ds(base, keys)
                for b in range(per):
                    here = pl.ds(base + b * LANES, LANES)
                    row = pl.ds(j * per + b, 1)
                    probs = weights_buf[here, cols] * scales[row, cols]
                    grad_probs = grad_buf[here, cols]
                    low_buf[here, cols] = probs.astype(bf16)
                    mixed_buf[here, cols] = (probs * grad_probs).astype(bf16)
                    scores_grad_buf[here, cols] = (probs * (grad_probs - row_dot)).astype(bf16)
                dv_acc[rng, :] += jnp.dot(low_buf[rng, cols], grads, preferred_element_type=f32)
                dk_acc[rng, :] += jnp.dot(
                    scores_grad_buf[rng, cols], qn, preferred_element_type=f32
                )

            over_keys(second)
            weighted_grad = jnp.dot(kn_t[...], mixed_buf[:, cols], preferred_element_type=f32)
            weighted_keys = jnp.dot(kn_t[...], low_buf[:, cols], preferred_element_type=f32)
            grad_q = ((weighted_grad - row_dot * weighted_keys) * factor).T
            result, text_sum, image_sum = finish(grad_q, unit, inverse, text, gains)
            dq_buf[at, :] = result
            gain_mine[0:1, :] += text_sum
            gain_mine[1:2, :] += image_sum

        def send_range(begin, end, flip):
            @pl.loop(begin, end)
            def _(k):
                send_back(0, real(jnp.where(flip, n - 1 - k, k), n))

        def place(i):
            down = jnp.logical_and(turn, i >= half)
            return down, jnp.where(down, i - half, i)

        def send_done(i):
            down, t = place(i)
            send_range((CHUNK * t) // rows, (CHUNK * (t + 1)) // rows, down)

        @pl.loop(0, full)
        def _(i):
            down, t = place(i)
            need = (CHUNK * (t + 1) - 1) // rows + 1
            had = jnp.where(t == 0, 0, (CHUNK * t - 1) // rows + 1)
            need = jnp.where(down, jnp.minimum(need, n - half_need), need)

            @pl.loop(had, need)
            def _(k):
                src = real(jnp.where(down, n - 1 - k, k), n)
                wait_in(2, src)
                wait_in(3, src)

            @pl.when(i == full - 1)
            def _():
                @pl.loop(0, full - 1)
                def _(k):
                    send_done(k)

            begin = jnp.where(down, total - CHUNK * (t + 1), CHUNK * t)
            attend(jnp.where(low, begin, total - CHUNK - begin), CHUNK)
            @pl.when(i == full - 1)
            def _():
                send_done(i)

        if tail:
            had_all = (CHUNK * full - 1) // rows + 1
            left_had = (CHUNK * (full - half) - 1) // rows + 1
            seen = jnp.where(turn, jnp.minimum(half_need + left_had, n), had_all)

            @pl.loop(seen, n)
            def _(k):
                k = jnp.where(turn, half_need + k - seen, k)
                wait_in(2, real(k, n))
                wait_in(3, real(k, n))

            begin = jnp.where(turn, CHUNK * half, CHUNK * full)
            attend(jnp.where(low, begin, total - tail - begin), tail)
        send_range(
            jnp.where(turn, half_done, (CHUNK * full) // rows),
            jnp.where(turn, n - rest_done, n),
            False,
        )

        @pl.loop(0, tiles)
        def _(c):
            at = pl.ds(pl.multiple_of(c * LANES, LANES), LANES)
            text, gains = gains_at(kg_ref, c * LANES, LANES)
            unit, inverse = unit_of(k_all[at, :])
            result, text_sum, image_sum = finish(
                dk_acc[at, :] * factor, unit, inverse, text, gains
            )
            dk_buf[at, :] = result
            gain_mine[2:3, :] += text_sum
            gain_mine[3:4, :] += image_sum

        @pl.loop(1, n)
        def _(s):
            gain_copy(partner(me, s, n)).start()

        pltpu.make_async_copy(gain_mine, gain_heads.at[mine], g1_recv.at[mine]).start()

        dv_buf[...] = dv_acc[...].astype(bf16)

        def far_first(s):
            return jnp.where(low, n - 1 - s, s)

        @pl.loop(0, n)
        def _(s):
            send_back(2, far_first(s))

        @pl.loop(0, n)
        def _(s):
            send_back(1, far_first(s))

    for h in range(heads):
        pltpu.make_async_copy(gain_mine, gain_heads.at[h], g1_recv.at[h]).wait()
    group = gain_heads[0]
    for h in range(1, heads):
        group = group + gain_heads[h]
    gain_group[...] = group
    for s in range(1, n_uly):
        uly_copy(s).start()
    gain_uly[uly] = group
    for s in range(1, n_uly):
        src = (uly + s) % n_uly
        pltpu.make_async_copy(gain_group, gain_uly.at[src], g2_recv.at[src]).wait()
    summed = gain_uly[0]
    for u in range(1, n_uly):
        summed = summed + gain_uly[u]
    q_gain_out[...] = summed[0:2, :]
    k_gain_out[...] = summed[2:4, :]

    for s in range(1, n_uly):
        uly_copy(s).wait_send()

    for a in range(3):
        for h in range(heads):
            pltpu.make_async_copy(
                backs[a].at[block(0)], outs[a].at[h], back_recv.at[a, h]
            ).wait()

    @pl.when(i_own)
    def _():
        @pl.loop(1, n)
        def _(s):
            gain_copy(partner(me, s, n)).wait_send()

        @pl.loop(1, n)
        def _(s):
            dev = partner(me, s, n)
            for a in range(3):
                back_copy(a, dev).wait_send()

    @pl.loop(1, n)
    def _(s):
        dev = partner(me, s, n)

        @pl.when(owns(dev))
        def _():
            for a in range(4):
                in_copy(a, s, head_of(dev), dev).wait_send()


def store(*refs):
    count = len(refs) // 2
    sems = refs[-1]
    copies = [
        pltpu.make_async_copy(refs[i], refs[count + i], sems.at[i]) for i in range(count)
    ]
    for copy in copies:
        copy.start()
    for copy in copies:
        copy.wait()


def solution(mesh):
    n, n_uly = mesh.shape["blk"], mesh.shape["uly"]

    def local(q_raw, k_raw, values, out_grad, q_gain, k_gain):
        rows, heads, width = q_raw.shape
        total = n * rows
        vmem = pl.BlockSpec(memory_space=pltpu.VMEM)
        first = [jnp.transpose(x, (1, 0, 2)) for x in (k_raw, values, q_raw, out_grad)]
        out_block = jax.ShapeDtypeStruct((heads, rows, width), bf16)
        hbm = pl.BlockSpec(memory_space=pltpu.HBM)
        gain_block = jax.ShapeDtypeStruct((2, width), f32)
        shapes = (out_block,) * 3 + (gain_block,) * 2
        held = tuple(pltpu.VMEM(x.shape, x.dtype) for x in shapes)
        results = pl.pallas_call(
            functools.partial(kernel, n, n_uly, heads, rows),
            out_shape=held,
            in_specs=[hbm] * 6,
            out_specs=(vmem,) * 5,
            scratch_shapes=[pltpu.VMEM((heads, rows, width), bf16)] * 4
            + [pltpu.VMEM((total, width), bf16)] * 5
            + [pltpu.VMEM((width, total), bf16)]
            + [pltpu.VMEM((total, width), f32)] * 2
            + [pltpu.VMEM((total, width), bf16)] * 3
            + [pltpu.VMEM((total, CHUNK), f32)] * 2
            + [pltpu.VMEM((total, CHUNK), bf16)] * 3
            + [pltpu.VMEM((total // LANES, CHUNK), f32)] * 4
            + [
                pltpu.VMEM((2, width), f32),
                pltpu.VMEM((2, width), f32),
                pltpu.VMEM((4, width), f32),
                pltpu.VMEM((heads, 4, width), f32),
                pltpu.VMEM((4, width), f32),
                pltpu.VMEM((n_uly, 4, width), f32),
                pltpu.SemaphoreType.DMA((6,)),
                pltpu.SemaphoreType.DMA((4, n)),
                pltpu.SemaphoreType.DMA((4, n)),
                pltpu.SemaphoreType.DMA((3, n)),
                pltpu.SemaphoreType.DMA((3, heads)),
                pltpu.SemaphoreType.DMA((n,)),
                pltpu.SemaphoreType.DMA((heads,)),
                pltpu.SemaphoreType.DMA((n_uly,)),
                pltpu.SemaphoreType.DMA((n_uly,)),
                pltpu.SemaphoreType.REGULAR,
            ],
            compiler_params=pltpu.CompilerParams(
                collective_id=0, has_side_effects=True, vmem_limit_bytes=KERNEL_VMEM
            ),
        )(*[pltpu.with_memory_space_constraint(x, pltpu.HBM) for x in (*first, q_gain, k_gain)])
        dq, dk, dv, q_total, k_total = pl.pallas_call(
            store,
            out_shape=shapes,
            in_specs=[vmem] * 5,
            out_specs=(hbm,) * 5,
            scratch_shapes=[pltpu.SemaphoreType.DMA((5,))],
            compiler_params=pltpu.CompilerParams(vmem_limit_bytes=STORE_VMEM),
        )(*results)
        back = [jnp.transpose(x, (1, 0, 2)) for x in (dq, dk, dv)]
        return (*back, q_total, k_total)

    placed = (P("blk", "uly", None),) * 4 + (P(), P())
    return jax.shard_map(
        local,
        mesh=mesh,
        in_specs=placed,
        out_specs=(P("blk", "uly", None),) * 3 + (P(), P()),
        check_vma=False,
    )
```

```python
import functools
import math

import jax
import jax.numpy as jnp
from jax import lax
from jax.experimental import pallas as pl
from jax.experimental.pallas import tpu as pltpu
from jax.sharding import PartitionSpec as P

TXT = 512
EPS = 1e-06
LANES = 128
CHUNK = 256
KEYS = 1152
KERNEL_VMEM = 48 * 2**20
STORE_VMEM = 2**20
MESH = pl.DeviceIdType.MESH
f32, bf16 = jnp.float32, jnp.bfloat16


def partner(me, step, n):
    if n & (n - 1):
        return (me + step) % n
    out, bit = 0, 1
    while bit < n:
        out = out + ((me // bit + step // bit) % 2) * bit
        bit *= 2
    return out


def kernel(
    n, n_uly, heads, rows,
    k_hbm, v_hbm, q_hbm, g_hbm, qg_hbm, kg_hbm,
    dq_out, dk_out, dv_out, q_gain_out, k_gain_out,
    k_in, v_in, q_in, g_in,
    k_all, v_all, q_all, g_all, kn, kn_t, dk_acc, dv_acc, dq_buf, dk_buf, dv_buf,
    weights_buf, grad_buf, low_buf, mixed_buf, scores_grad_buf, peaks, sums, dots, scales,
    qg_ref, kg_ref, gain_mine, gain_heads, gain_group, gain_uly,
    staged, in_send, in_recv, back_send, back_recv, g1_send, g1_recv, g2_send, g2_recv, entered,
):
    me = lax.axis_index("blk")
    uly = lax.axis_index("uly")
    total = n * rows
    full = total // CHUNK
    tail = total - full * CHUNK
    tiles = total // LANES
    unroll = max(u for u in range(1, 10) if tiles % u == 0)
    width = k_in.shape[2]
    factor = 1.0 / math.sqrt(width)
    factor2 = factor * math.log2(math.e)
    keys = max(d for d in range(LANES, min(total, KEYS) + 1, LANES) if total % d == 0)
    phase = (uly % 2) * (heads % n)

    def head_of(dev):
        return (heads * dev + phase) // n

    def owns(dev):
        return (heads * dev + phase) % n + heads >= n

    def owner(h):
        return ((h + 1) * n - phase + heads - 1) // heads - 1

    mine = head_of(me)
    i_own = owns(me)

    sources = (k_hbm, v_hbm, q_hbm, g_hbm)
    ins = (k_in, v_in, q_in, g_in)
    alls = (k_all, v_all, q_all, g_all)
    backs = (dq_buf, dk_buf, dv_buf)
    outs = (dq_out, dk_out, dv_out)

    def block(dev):
        return pl.ds(pl.multiple_of(dev * rows, 16), rows)

    def stage(a):
        return pltpu.make_async_copy(sources[a], ins[a], staged.at[a])

    gain_stages = (
        pltpu.make_async_copy(qg_hbm, qg_ref, staged.at[4]),
        pltpu.make_async_copy(kg_hbm, kg_ref, staged.at[5]),
    )

    quarter = n // 4

    def inner(dev):
        return jnp.logical_and(dev >= quarter, dev < n - quarter)

    i_inner = inner(me)
    pair = jnp.where((me // quarter) % 2 == 0, me + quarter, me - quarter)
    barrier = pltpu.get_barrier_semaphore()
    for s in range(1, n_uly):
        pl.semaphore_signal(
            barrier, inc=1, device_id={"uly": (uly + s) % n_uly}, device_id_type=MESH
        )

    @pl.when(i_inner)
    def _():
        @pl.loop(quarter, n - quarter)
        def _(dev):
            @pl.when(dev != me)
            def _():
                pl.semaphore_signal(barrier, inc=1, device_id={"blk": dev}, device_id_type=MESH)

    for a in range(4):
        stage(a).start()
    for copy in gain_stages:
        copy.start()

    @pl.when(i_inner)
    def _():
        pl.semaphore_wait(barrier, n - 2 * quarter - 1 + n_uly - 1)
        pl.semaphore_signal(barrier, inc=1, device_id={"blk": pair}, device_id_type=MESH)

    @pl.when(jnp.logical_not(i_inner))
    def _():
        pl.semaphore_wait(barrier, 1 + n_uly - 1)

        @pl.loop(quarter, n - quarter)
        def _(dev):
            pl.semaphore_signal(entered, inc=1, device_id={"blk": dev}, device_id_type=MESH)

    def meet():
        @pl.when(i_inner)
        def _():
            pl.semaphore_wait(entered, 2 * quarter)
            pl.semaphore_signal(entered, inc=1, device_id={"blk": pair}, device_id_type=MESH)

        @pl.when(jnp.logical_not(i_inner))
        def _():
            pl.semaphore_wait(entered, 1)

    def in_copy(a, s, h, dev):
        return pltpu.make_async_remote_copy(
            src_ref=ins[a].at[h], dst_ref=alls[a].at[block(me)],
            send_sem=in_send.at[a, s], recv_sem=in_recv.at[a, me],
            device_id={"blk": dev}, device_id_type=MESH,
        )

    def send_in(a, s, near=None):
        dev = partner(me, s, n)
        wanted = owns(dev)
        if near is not None:
            wanted = jnp.logical_and(wanted, inner(dev) == near)

        @pl.when(wanted)
        def _():
            in_copy(a, s, head_of(dev), dev).start()

    def keep_in(a):
        @pl.when(i_own)
        def _():
            pltpu.make_async_copy(
                ins[a].at[mine], alls[a].at[block(me)], in_recv.at[a, me]
            ).start()

    def wait_in(a, src):
        pltpu.make_async_copy(ins[a].at[0], alls[a].at[block(src)], in_recv.at[a, src]).wait()

    for first in (True, False):
        for a in (0, 1):
            if first:
                stage(a).wait()
            for s in range(n - 1, 0, -1):
                send_in(a, s, first)
        if first:
            meet()
    for a in (2, 3):
        stage(a).wait()
    for copy in gain_stages:
        copy.wait()
    for a in range(4):
        keep_in(a)
    for s in range(1, n):
        for a in (2, 3):
            send_in(a, s)

    def back_copy(a, dev):
        return pltpu.make_async_remote_copy(
            src_ref=backs[a].at[block(dev)], dst_ref=outs[a].at[mine],
            send_sem=back_send.at[a, dev], recv_sem=back_recv.at[a, mine],
            device_id={"blk": dev}, device_id_type=MESH,
        )

    def send_back(a, dev):
        @pl.when(dev != me)
        def _():
            back_copy(a, dev).start()

        @pl.when(dev == me)
        def _():
            pltpu.make_async_copy(
                backs[a].at[block(dev)], outs[a].at[mine], back_recv.at[a, mine]
            ).start()

    def gain_copy(dev):
        return pltpu.make_async_remote_copy(
            src_ref=gain_mine, dst_ref=gain_heads.at[mine],
            send_sem=g1_send.at[dev], recv_sem=g1_recv.at[mine],
            device_id={"blk": dev}, device_id_type=MESH,
        )

    def uly_copy(s):
        return pltpu.make_async_remote_copy(
            src_ref=gain_group, dst_ref=gain_uly.at[uly],
            send_sem=g2_send.at[s], recv_sem=g2_recv.at[uly],
            device_id={"uly": (uly + s) % n_uly}, device_id_type=MESH,
        )

    def gains_at(gain_ref, base, size):
        position = base + lax.broadcasted_iota(jnp.int32, (size, width), 0)
        text = position < TXT
        return text, jnp.where(text, gain_ref[0:1, :], gain_ref[1:2, :])

    def unit_of(raw):
        wide = raw.astype(f32)
        inverse = lax.rsqrt(jnp.mean(wide * wide, axis=-1, keepdims=True) + EPS)
        return wide * inverse, inverse

    def finish(grad, unit, inverse, text, gains):
        part = grad * unit
        scaled = grad * gains
        text_sum = jnp.sum(jnp.where(text, part, 0.0), axis=0, keepdims=True)
        image_sum = jnp.sum(jnp.where(text, 0.0, part), axis=0, keepdims=True)
        result = (scaled - unit * jnp.mean(scaled * unit, axis=-1, keepdims=True)) * inverse
        return result.astype(bf16), text_sum, image_sum

    @pl.when(i_own)
    def _():
        low = me < n // 2
        turn = jnp.where(low, me, n - 1 - me) >= n // 4
        half = full // 2
        half_need = (CHUNK * half - 1) // rows + 1
        half_done = (CHUNK * half) // rows
        rest_done = (CHUNK * (full - half)) // rows
        nt = (((1,), (1,)), ((), ()))

        def real(i, count):
            return jnp.where(low, i, count - 1 - i)

        gain_mine[...] = jnp.zeros_like(gain_mine)
        dk_acc[...] = jnp.zeros_like(dk_acc)
        dv_acc[...] = jnp.zeros_like(dv_acc)

        @pl.loop(0, n)
        def _(src):
            wait_in(0, src)

        @pl.loop(0, tiles, unroll=unroll)
        def _(c):
            at = pl.ds(pl.multiple_of(c * LANES, LANES), LANES)
            text, gains = gains_at(kg_ref, c * LANES, LANES)
            unit, _inverse = unit_of(k_all[at, :])
            normed = unit * gains
            kn[at, :] = normed.astype(bf16)
            kn_t[:, at] = normed.T.astype(bf16)

        @pl.loop(0, n)
        def _(src):
            wait_in(1, src)

        def over_keys(body):
            if keys == total:
                body(0)
            else:
                @pl.loop(0, total // keys)
                def _(j):
                    body(j)

        def attend(start, size):
            start = pl.multiple_of(start, LANES)
            at = pl.ds(start, size)
            text, gains = gains_at(qg_ref, start, size)
            unit, inverse = unit_of(q_all[at, :])
            qn = (unit * gains).astype(bf16)
            grads = g_all[at, :]
            cols = pl.ds(0, size)
            per = keys // LANES

            def first(j):
                base = pl.multiple_of(j * keys, LANES)
                rng = pl.ds(base, keys)
                scores = lax.dot_general(kn[rng, :], qn, nt, preferred_element_type=f32)
                grad_probs = lax.dot_general(v_all[rng, :], grads, nt, preferred_element_type=f32)
                for b in range(per):
                    part = slice(b * LANES, (b + 1) * LANES)
                    here = pl.ds(base + b * LANES, LANES)
                    row = pl.ds(j * per + b, 1)
                    peak = jnp.max(scores[part], axis=0, keepdims=True)
                    weights = jnp.exp2((scores[part] - peak) * factor2)
                    peaks[row, cols] = peak
                    sums[row, cols] = jnp.sum(weights, axis=0, keepdims=True)
                    dots[row, cols] = jnp.sum(weights * grad_probs[part], axis=0, keepdims=True)
                    weights_buf[here, cols] = weights
                    grad_buf[here, cols] = grad_probs[part]

            over_keys(first)
            peak_all = peaks[:, cols]
            lift = jnp.exp2((peak_all - jnp.max(peak_all, axis=0, keepdims=True)) * factor2)
            inverse_total = 1.0 / jnp.sum(lift * sums[:, cols], axis=0, keepdims=True)
            row_dot = jnp.sum(lift * dots[:, cols], axis=0, keepdims=True) * inverse_total
            scales[:, cols] = lift * inverse_total

            def second(j):
                base = pl.multiple_of(j * keys, LANES)
                rng = pl.ds(base, keys)
                for b in range(per):
                    here = pl.ds(base + b * LANES, LANES)
                    row = pl.ds(j * per + b, 1)
                    probs = weights_buf[here, cols] * scales[row, cols]
                    grad_probs = grad_buf[here, cols]
                    low_buf[here, cols] = probs.astype(bf16)
                    mixed_buf[here, cols] = (probs * grad_probs).astype(bf16)
                    scores_grad_buf[here, cols] = (probs * (grad_probs - row_dot)).astype(bf16)
                dv_acc[rng, :] += jnp.dot(low_buf[rng, cols], grads, preferred_element_type=f32)
                dk_acc[rng, :] += jnp.dot(
                    scores_grad_buf[rng, cols], qn, preferred_element_type=f32
                )

            over_keys(second)
            weighted_grad = jnp.dot(kn_t[...], mixed_buf[:, cols], preferred_element_type=f32)
            weighted_keys = jnp.dot(kn_t[...], low_buf[:, cols], preferred_element_type=f32)
            grad_q = ((weighted_grad - row_dot * weighted_keys) * factor).T
            result, text_sum, image_sum = finish(grad_q, unit, inverse, text, gains)
            dq_buf[at, :] = result
            gain_mine[0:1, :] += text_sum
            gain_mine[1:2, :] += image_sum

        def send_range(begin, end, flip):
            @pl.loop(begin, end)
            def _(k):
                send_back(0, real(jnp.where(flip, n - 1 - k, k), n))

        def place(i):
            down = jnp.logical_and(turn, i >= half)
            return down, jnp.where(down, i - half, i)

        def send_done(i):
            down, t = place(i)
            send_range((CHUNK * t) // rows, (CHUNK * (t + 1)) // rows, down)

        @pl.loop(0, full)
        def _(i):
            down, t = place(i)
            need = (CHUNK * (t + 1) - 1) // rows + 1
            had = jnp.where(t == 0, 0, (CHUNK * t - 1) // rows + 1)
            need = jnp.where(down, jnp.minimum(need, n - half_need), need)

            @pl.loop(had, need)
            def _(k):
                src = real(jnp.where(down, n - 1 - k, k), n)
                wait_in(2, src)
                wait_in(3, src)

            @pl.when(i == full - 1)
            def _():
                @pl.loop(0, full - 1)
                def _(k):
                    send_done(k)

            begin = jnp.where(down, total - CHUNK * (t + 1), CHUNK * t)
            attend(jnp.where(low, begin, total - CHUNK - begin), CHUNK)
            @pl.when(i == full - 1)
            def _():
                send_done(i)

        if tail:
            had_all = (CHUNK * full - 1) // rows + 1
            left_had = (CHUNK * (full - half) - 1) // rows + 1
            seen = jnp.where(turn, jnp.minimum(half_need + left_had, n), had_all)

            @pl.loop(seen, n)
            def _(k):
                k = jnp.where(turn, half_need + k - seen, k)
                wait_in(2, real(k, n))
                wait_in(3, real(k, n))

            begin = jnp.where(turn, CHUNK * half, CHUNK * full)
            attend(jnp.where(low, begin, total - tail - begin), tail)
        send_range(
            jnp.where(turn, half_done, (CHUNK * full) // rows),
            jnp.where(turn, n - rest_done, n),
            False,
        )

        @pl.loop(0, tiles, unroll=unroll)
        def _(c):
            at = pl.ds(pl.multiple_of(c * LANES, LANES), LANES)
            text, gains = gains_at(kg_ref, c * LANES, LANES)
            unit, inverse = unit_of(k_all[at, :])
            result, text_sum, image_sum = finish(
                dk_acc[at, :] * factor, unit, inverse, text, gains
            )
            dk_buf[at, :] = result
            gain_mine[2:3, :] += text_sum
            gain_mine[3:4, :] += image_sum

        @pl.loop(1, n)
        def _(s):
            gain_copy(partner(me, s, n)).start()

        pltpu.make_async_copy(gain_mine, gain_heads.at[mine], g1_recv.at[mine]).start()

        dv_buf[...] = dv_acc[...].astype(bf16)

        side = n // 2

        def spread(j):
            return jnp.where(j < quarter, 2 * j, 2 * (j - quarter) + 1)

        def target(s):
            crossing = jnp.logical_and(s > 0, s <= side)
            ahead = jnp.where(crossing, side + spread(s - 1), spread(s % side))
            behind = jnp.where(s < side, spread(s), side + spread(s - side))
            return jnp.where(low, ahead, behind)

        for a in (2, 1):
            send_back(a, target(0))

        @pl.loop(1, n)
        def _(s):
            send_back(2, target(s))

        @pl.loop(1, n)
        def _(s):
            send_back(1, target(s))

    @pl.loop(1, n)
    def _(s):
        dev = partner(me, s, n)

        @pl.when(owns(dev))
        def _():
            for a in range(4):
                in_copy(a, s, head_of(dev), dev).wait_send()

    for h in range(heads):
        pltpu.make_async_copy(gain_mine, gain_heads.at[h], g1_recv.at[h]).wait()
    group = gain_heads[0]
    for h in range(1, heads):
        group = group + gain_heads[h]
    gain_group[...] = group
    for s in range(1, n_uly):
        uly_copy(s).start()
    gain_uly[uly] = group
    for s in range(1, n_uly):
        src = (uly + s) % n_uly
        pltpu.make_async_copy(gain_group, gain_uly.at[src], g2_recv.at[src]).wait()
    summed = gain_uly[0]
    for u in range(1, n_uly):
        summed = summed + gain_uly[u]
    q_gain_out[...] = summed[0:2, :]
    k_gain_out[...] = summed[2:4, :]

    for s in range(1, n_uly):
        uly_copy(s).wait_send()

    def wait_back(a):
        for h in range(heads):
            pltpu.make_async_copy(backs[a].at[block(0)], outs[a].at[h], back_recv.at[a, h]).wait()

    wait_back(0)
    wait_back(2)

    @pl.when(i_own)
    def _():
        @pl.loop(1, n)
        def _(s):
            gain_copy(partner(me, s, n)).wait_send()

        @pl.loop(1, n)
        def _(s):
            dev = partner(me, s, n)
            for a in range(3):
                back_copy(a, dev).wait_send()

    wait_back(1)


def store(*refs):
    count = len(refs) // 2
    sems = refs[-1]
    copies = [
        pltpu.make_async_copy(refs[i], refs[count + i], sems.at[i]) for i in range(count)
    ]
    for copy in copies:
        copy.start()
    for copy in copies:
        copy.wait()


def solution(mesh):
    n, n_uly = mesh.shape["blk"], mesh.shape["uly"]

    def local(q_raw, k_raw, values, out_grad, q_gain, k_gain):
        rows, heads, width = q_raw.shape
        total = n * rows
        vmem = pl.BlockSpec(memory_space=pltpu.VMEM)
        first = [jnp.transpose(x, (1, 0, 2)) for x in (k_raw, values, q_raw, out_grad)]
        out_block = jax.ShapeDtypeStruct((heads, rows, width), bf16)
        hbm = pl.BlockSpec(memory_space=pltpu.HBM)
        gain_block = jax.ShapeDtypeStruct((2, width), f32)
        shapes = (out_block,) * 3 + (gain_block,) * 2
        held = tuple(pltpu.VMEM(x.shape, x.dtype) for x in shapes)
        results = pl.pallas_call(
            functools.partial(kernel, n, n_uly, heads, rows),
            out_shape=held,
            in_specs=[hbm] * 6,
            out_specs=(vmem,) * 5,
            scratch_shapes=[pltpu.VMEM((heads, rows, width), bf16)] * 4
            + [pltpu.VMEM((total, width), bf16)] * 5
            + [pltpu.VMEM((width, total), bf16)]
            + [pltpu.VMEM((total, width), f32)] * 2
            + [pltpu.VMEM((total, width), bf16)] * 3
            + [pltpu.VMEM((total, CHUNK), f32)] * 2
            + [pltpu.VMEM((total, CHUNK), bf16)] * 3
            + [pltpu.VMEM((total // LANES, CHUNK), f32)] * 4
            + [
                pltpu.VMEM((2, width), f32),
                pltpu.VMEM((2, width), f32),
                pltpu.VMEM((4, width), f32),
                pltpu.VMEM((heads, 4, width), f32),
                pltpu.VMEM((4, width), f32),
                pltpu.VMEM((n_uly, 4, width), f32),
                pltpu.SemaphoreType.DMA((6,)),
                pltpu.SemaphoreType.DMA((4, n)),
                pltpu.SemaphoreType.DMA((4, n)),
                pltpu.SemaphoreType.DMA((3, n)),
                pltpu.SemaphoreType.DMA((3, heads)),
                pltpu.SemaphoreType.DMA((n,)),
                pltpu.SemaphoreType.DMA((heads,)),
                pltpu.SemaphoreType.DMA((n_uly,)),
                pltpu.SemaphoreType.DMA((n_uly,)),
                pltpu.SemaphoreType.REGULAR,
            ],
            compiler_params=pltpu.CompilerParams(
                collective_id=0, has_side_effects=True, vmem_limit_bytes=KERNEL_VMEM
            ),
        )(*[pltpu.with_memory_space_constraint(x, pltpu.HBM) for x in (*first, q_gain, k_gain)])
        dq, dk, dv, q_total, k_total = pl.pallas_call(
            store,
            out_shape=shapes,
            in_specs=[vmem] * 5,
            out_specs=(hbm,) * 5,
            scratch_shapes=[pltpu.SemaphoreType.DMA((5,))],
            compiler_params=pltpu.CompilerParams(vmem_limit_bytes=STORE_VMEM),
        )(*results)
        back = [jnp.transpose(x, (1, 0, 2)) for x in (dq, dk, dv)]
        return (*back, q_total, k_total)

    placed = (P("blk", "uly", None),) * 4 + (P(), P())
    return jax.shard_map(
        local,
        mesh=mesh,
        in_specs=placed,
        out_specs=(P("blk", "uly", None),) * 3 + (P(), P()),
        check_vma=False,
    )
```

```python
import functools
import math

import jax
import jax.numpy as jnp
from jax import lax
from jax.experimental import pallas as pl
from jax.experimental.pallas import tpu as pltpu
from jax.sharding import PartitionSpec as P

TXT = 512
EPS = 1e-06
LANES = 128
CHUNK = 256
KEYS = 1152
KERNEL_VMEM = 48 * 2**20
STORE_VMEM = 2**20
MESH = pl.DeviceIdType.MESH
f32, bf16 = jnp.float32, jnp.bfloat16


def partner(me, step, n):
    if n & (n - 1):
        return (me + step) % n
    out, bit = 0, 1
    while bit < n:
        out = out + ((me // bit + step // bit) % 2) * bit
        bit *= 2
    return out


def kernel(
    n, n_uly, heads, rows,
    k_hbm, v_hbm, q_hbm, g_hbm, qg_hbm, kg_hbm,
    dq_out, dk_out, dv_out, q_gain_out, k_gain_out,
    k_in, v_in, q_in, g_in,
    k_all, v_all, q_all, g_all, kn, kn_t, dk_acc, dv_acc, dq_buf, dk_buf, dv_buf,
    weights_buf, grad_buf, low_buf, mixed_buf, scores_grad_buf, peaks, sums, dots, scales,
    qg_ref, kg_ref, gain_mine, gain_heads, gain_group, gain_uly,
    staged, in_send, in_recv, back_send, back_recv, g1_send, g1_recv, g2_send, g2_recv, entered,
):
    me = lax.axis_index("blk")
    uly = lax.axis_index("uly")
    total = n * rows
    full = total // CHUNK
    tail = total - full * CHUNK
    tiles = total // LANES
    unroll = max(u for u in range(1, 10) if tiles % u == 0)
    width = k_in.shape[2]
    factor = 1.0 / math.sqrt(width)
    factor2 = factor * math.log2(math.e)
    keys = max(d for d in range(LANES, min(total, KEYS) + 1, LANES) if total % d == 0)
    def rank(dev):
        side = n // 2
        turned = jnp.where(dev < side, dev, n - 1 + side - dev)
        return jnp.where(uly % 2 == 0, turned, turned + 1 - 2 * (turned % 2))

    def head_of(dev):
        return (heads * rank(dev)) // n

    def owns(dev):
        return (heads * rank(dev)) % n + heads >= n

    mine = head_of(me)
    i_own = owns(me)

    sources = (k_hbm, v_hbm, q_hbm, g_hbm)
    ins = (k_in, v_in, q_in, g_in)
    alls = (k_all, v_all, q_all, g_all)
    backs = (dq_buf, dk_buf, dv_buf)
    outs = (dq_out, dk_out, dv_out)

    def block(dev):
        return pl.ds(pl.multiple_of(dev * rows, 16), rows)

    def stage(a):
        return pltpu.make_async_copy(sources[a], ins[a], staged.at[a])

    gain_stages = (
        pltpu.make_async_copy(qg_hbm, qg_ref, staged.at[4]),
        pltpu.make_async_copy(kg_hbm, kg_ref, staged.at[5]),
    )

    quarter = n // 4

    def inner(dev):
        return jnp.logical_and(dev >= quarter, dev < n - quarter)

    i_inner = inner(me)
    pair = jnp.where((me // quarter) % 2 == 0, me + quarter, me - quarter)
    barrier = pltpu.get_barrier_semaphore()
    for s in range(1, n_uly):
        pl.semaphore_signal(
            barrier, inc=1, device_id={"uly": (uly + s) % n_uly}, device_id_type=MESH
        )

    @pl.when(i_inner)
    def _():
        @pl.loop(quarter, n - quarter)
        def _(dev):
            @pl.when(dev != me)
            def _():
                pl.semaphore_signal(barrier, inc=1, device_id={"blk": dev}, device_id_type=MESH)

    for a in range(4):
        stage(a).start()
    for copy in gain_stages:
        copy.start()

    @pl.when(i_inner)
    def _():
        pl.semaphore_wait(barrier, n - 2 * quarter - 1 + n_uly - 1)
        pl.semaphore_signal(barrier, inc=1, device_id={"blk": pair}, device_id_type=MESH)

    @pl.when(jnp.logical_not(i_inner))
    def _():
        pl.semaphore_wait(barrier, 1 + n_uly - 1)

        @pl.loop(quarter, n - quarter)
        def _(dev):
            pl.semaphore_signal(entered, inc=1, device_id={"blk": dev}, device_id_type=MESH)

    def meet():
        @pl.when(i_inner)
        def _():
            pl.semaphore_wait(entered, 2 * quarter)
            pl.semaphore_signal(entered, inc=1, device_id={"blk": pair}, device_id_type=MESH)

        @pl.when(jnp.logical_not(i_inner))
        def _():
            pl.semaphore_wait(entered, 1)

    def in_copy(a, s, h, dev):
        return pltpu.make_async_remote_copy(
            src_ref=ins[a].at[h], dst_ref=alls[a].at[block(me)],
            send_sem=in_send.at[a, s], recv_sem=in_recv.at[a, me],
            device_id={"blk": dev}, device_id_type=MESH,
        )

    def send_in(a, s, near=None):
        dev = partner(me, s, n)
        wanted = owns(dev)
        if near is not None:
            wanted = jnp.logical_and(wanted, inner(dev) == near)

        @pl.when(wanted)
        def _():
            in_copy(a, s, head_of(dev), dev).start()

    def keep_in(a):
        @pl.when(i_own)
        def _():
            pltpu.make_async_copy(
                ins[a].at[mine], alls[a].at[block(me)], in_recv.at[a, me]
            ).start()

    def wait_in(a, src):
        pltpu.make_async_copy(ins[a].at[0], alls[a].at[block(src)], in_recv.at[a, src]).wait()

    for first in (True, False):
        for a in (0, 1):
            if first:
                stage(a).wait()
            for s in range(n - 1, 0, -1):
                send_in(a, s, first)
        if first:
            meet()
    for a in (2, 3):
        stage(a).wait()
    for copy in gain_stages:
        copy.wait()
    for a in range(4):
        keep_in(a)
    for s in range(1, n):
        for a in (2, 3):
            send_in(a, s)

    def back_copy(a, dev):
        return pltpu.make_async_remote_copy(
            src_ref=backs[a].at[block(dev)], dst_ref=outs[a].at[mine],
            send_sem=back_send.at[a, dev], recv_sem=back_recv.at[a, mine],
            device_id={"blk": dev}, device_id_type=MESH,
        )

    def send_back(a, dev):
        @pl.when(dev != me)
        def _():
            back_copy(a, dev).start()

        @pl.when(dev == me)
        def _():
            pltpu.make_async_copy(
                backs[a].at[block(dev)], outs[a].at[mine], back_recv.at[a, mine]
            ).start()

    def gain_copy(dev):
        return pltpu.make_async_remote_copy(
            src_ref=gain_mine, dst_ref=gain_heads.at[mine],
            send_sem=g1_send.at[dev], recv_sem=g1_recv.at[mine],
            device_id={"blk": dev}, device_id_type=MESH,
        )

    def uly_copy(s):
        return pltpu.make_async_remote_copy(
            src_ref=gain_group, dst_ref=gain_uly.at[uly],
            send_sem=g2_send.at[s], recv_sem=g2_recv.at[uly],
            device_id={"uly": (uly + s) % n_uly}, device_id_type=MESH,
        )

    def gains_at(gain_ref, base, size):
        position = base + lax.broadcasted_iota(jnp.int32, (size, width), 0)
        text = position < TXT
        return text, jnp.where(text, gain_ref[0:1, :], gain_ref[1:2, :])

    def unit_of(raw):
        wide = raw.astype(f32)
        inverse = lax.rsqrt(jnp.mean(wide * wide, axis=-1, keepdims=True) + EPS)
        return wide * inverse, inverse

    def finish(grad, unit, inverse, text, gains):
        part = grad * unit
        scaled = grad * gains
        text_sum = jnp.sum(jnp.where(text, part, 0.0), axis=0, keepdims=True)
        image_sum = jnp.sum(jnp.where(text, 0.0, part), axis=0, keepdims=True)
        result = (scaled - unit * jnp.mean(scaled * unit, axis=-1, keepdims=True)) * inverse
        return result.astype(bf16), text_sum, image_sum

    @pl.when(i_own)
    def _():
        low = me < n // 2
        turn = jnp.where(low, me, n - 1 - me) >= n // 4
        half = full // 2
        half_need = (CHUNK * half - 1) // rows + 1
        half_done = (CHUNK * half) // rows
        rest_done = (CHUNK * (full - half)) // rows
        nt = (((1,), (1,)), ((), ()))

        def real(i, count):
            return jnp.where(low, i, count - 1 - i)

        gain_mine[...] = jnp.zeros_like(gain_mine)
        dk_acc[...] = jnp.zeros_like(dk_acc)
        dv_acc[...] = jnp.zeros_like(dv_acc)

        @pl.loop(0, n)
        def _(src):
            wait_in(0, src)

        @pl.loop(0, tiles, unroll=unroll)
        def _(c):
            at = pl.ds(pl.multiple_of(c * LANES, LANES), LANES)
            text, gains = gains_at(kg_ref, c * LANES, LANES)
            unit, _inverse = unit_of(k_all[at, :])
            normed = unit * gains
            kn[at, :] = normed.astype(bf16)
            kn_t[:, at] = normed.T.astype(bf16)

        @pl.loop(0, n)
        def _(src):
            wait_in(1, src)

        def over_keys(body):
            if keys == total:
                body(0)
            else:
                @pl.loop(0, total // keys)
                def _(j):
                    body(j)

        def attend(start, size):
            start = pl.multiple_of(start, LANES)
            at = pl.ds(start, size)
            text, gains = gains_at(qg_ref, start, size)
            unit, inverse = unit_of(q_all[at, :])
            qn = (unit * gains).astype(bf16)
            grads = g_all[at, :]
            cols = pl.ds(0, size)
            per = keys // LANES

            def first(j):
                base = pl.multiple_of(j * keys, LANES)
                rng = pl.ds(base, keys)
                scores = lax.dot_general(kn[rng, :], qn, nt, preferred_element_type=f32)
                grad_probs = lax.dot_general(v_all[rng, :], grads, nt, preferred_element_type=f32)
                for b in range(per):
                    part = slice(b * LANES, (b + 1) * LANES)
                    here = pl.ds(base + b * LANES, LANES)
                    row = pl.ds(j * per + b, 1)
                    peak = jnp.max(scores[part], axis=0, keepdims=True)
                    weights = jnp.exp2((scores[part] - peak) * factor2)
                    peaks[row, cols] = peak
                    sums[row, cols] = jnp.sum(weights, axis=0, keepdims=True)
                    dots[row, cols] = jnp.sum(weights * grad_probs[part], axis=0, keepdims=True)
                    weights_buf[here, cols] = weights
                    grad_buf[here, cols] = grad_probs[part]

            over_keys(first)
            peak_all = peaks[:, cols]
            lift = jnp.exp2((peak_all - jnp.max(peak_all, axis=0, keepdims=True)) * factor2)
            inverse_total = 1.0 / jnp.sum(lift * sums[:, cols], axis=0, keepdims=True)
            row_dot = jnp.sum(lift * dots[:, cols], axis=0, keepdims=True) * inverse_total
            scales[:, cols] = lift * inverse_total

            def second(j):
                base = pl.multiple_of(j * keys, LANES)
                rng = pl.ds(base, keys)
                for b in range(per):
                    here = pl.ds(base + b * LANES, LANES)
                    row = pl.ds(j * per + b, 1)
                    probs = weights_buf[here, cols] * scales[row, cols]
                    grad_probs = grad_buf[here, cols]
                    low_buf[here, cols] = probs.astype(bf16)
                    mixed_buf[here, cols] = (probs * grad_probs).astype(bf16)
                    scores_grad_buf[here, cols] = (probs * (grad_probs - row_dot)).astype(bf16)
                dv_acc[rng, :] += jnp.dot(low_buf[rng, cols], grads, preferred_element_type=f32)
                dk_acc[rng, :] += jnp.dot(
                    scores_grad_buf[rng, cols], qn, preferred_element_type=f32
                )

            over_keys(second)
            weighted_grad = jnp.dot(kn_t[...], mixed_buf[:, cols], preferred_element_type=f32)
            weighted_keys = jnp.dot(kn_t[...], low_buf[:, cols], preferred_element_type=f32)
            grad_q = ((weighted_grad - row_dot * weighted_keys) * factor).T
            result, text_sum, image_sum = finish(grad_q, unit, inverse, text, gains)
            dq_buf[at, :] = result
            gain_mine[0:1, :] += text_sum
            gain_mine[1:2, :] += image_sum

        def send_range(begin, end, flip):
            @pl.loop(begin, end)
            def _(k):
                send_back(0, real(jnp.where(flip, n - 1 - k, k), n))

        def place(i):
            down = jnp.logical_and(turn, i >= half)
            return down, jnp.where(down, i - half, i)

        def send_done(i):
            down, t = place(i)
            send_range((CHUNK * t) // rows, (CHUNK * (t + 1)) // rows, down)

        @pl.loop(0, full)
        def _(i):
            down, t = place(i)
            need = (CHUNK * (t + 1) - 1) // rows + 1
            had = jnp.where(t == 0, 0, (CHUNK * t - 1) // rows + 1)
            need = jnp.where(down, jnp.minimum(need, n - half_need), need)

            @pl.loop(had, need)
            def _(k):
                src = real(jnp.where(down, n - 1 - k, k), n)
                wait_in(2, src)
                wait_in(3, src)

            @pl.when(i == full - 1)
            def _():
                @pl.loop(0, full - 1)
                def _(k):
                    send_done(k)

            begin = jnp.where(down, total - CHUNK * (t + 1), CHUNK * t)
            attend(jnp.where(low, begin, total - CHUNK - begin), CHUNK)
            @pl.when(i == full - 1)
            def _():
                send_done(i)

        if tail:
            had_all = (CHUNK * full - 1) // rows + 1
            left_had = (CHUNK * (full - half) - 1) // rows + 1
            seen = jnp.where(turn, jnp.minimum(half_need + left_had, n), had_all)

            @pl.loop(seen, n)
            def _(k):
                k = jnp.where(turn, half_need + k - seen, k)
                wait_in(2, real(k, n))
                wait_in(3, real(k, n))

            begin = jnp.where(turn, CHUNK * half, CHUNK * full)
            attend(jnp.where(low, begin, total - tail - begin), tail)
        send_range(
            jnp.where(turn, half_done, (CHUNK * full) // rows),
            jnp.where(turn, n - rest_done, n),
            False,
        )

        @pl.loop(0, tiles, unroll=unroll)
        def _(c):
            at = pl.ds(pl.multiple_of(c * LANES, LANES), LANES)
            text, gains = gains_at(kg_ref, c * LANES, LANES)
            unit, inverse = unit_of(k_all[at, :])
            result, text_sum, image_sum = finish(
                dk_acc[at, :] * factor, unit, inverse, text, gains
            )
            dk_buf[at, :] = result
            gain_mine[2:3, :] += text_sum
            gain_mine[3:4, :] += image_sum

        @pl.loop(1, n)
        def _(s):
            gain_copy(partner(me, s, n)).start()

        pltpu.make_async_copy(gain_mine, gain_heads.at[mine], g1_recv.at[mine]).start()

        dv_buf[...] = dv_acc[...].astype(bf16)

        side = n // 2

        def spread(j):
            return jnp.where(j < quarter, 2 * j, 2 * (j - quarter) + 1)

        def target(s):
            crossing = jnp.logical_and(s > 0, s <= side)
            ahead = jnp.where(crossing, side + spread(s - 1), spread(s % side))
            return jnp.where(low, ahead, s)

        for a in (2, 1):
            send_back(a, target(0))

        @pl.loop(1, n)
        def _(s):
            send_back(2, target(s))

        @pl.loop(1, n)
        def _(s):
            send_back(1, target(s))

    @pl.loop(1, n)
    def _(s):
        dev = partner(me, s, n)

        @pl.when(owns(dev))
        def _():
            for a in range(4):
                in_copy(a, s, head_of(dev), dev).wait_send()

    for h in range(heads):
        pltpu.make_async_copy(gain_mine, gain_heads.at[h], g1_recv.at[h]).wait()
    group = gain_heads[0]
    for h in range(1, heads):
        group = group + gain_heads[h]
    gain_group[...] = group
    for s in range(1, n_uly):
        uly_copy(s).start()
    gain_uly[uly] = group
    for s in range(1, n_uly):
        src = (uly + s) % n_uly
        pltpu.make_async_copy(gain_group, gain_uly.at[src], g2_recv.at[src]).wait()
    summed = gain_uly[0]
    for u in range(1, n_uly):
        summed = summed + gain_uly[u]
    q_gain_out[...] = summed[0:2, :]
    k_gain_out[...] = summed[2:4, :]

    for s in range(1, n_uly):
        uly_copy(s).wait_send()

    def wait_back(a):
        for h in range(heads):
            pltpu.make_async_copy(backs[a].at[block(0)], outs[a].at[h], back_recv.at[a, h]).wait()

    wait_back(0)
    wait_back(2)

    @pl.when(i_own)
    def _():
        @pl.loop(1, n)
        def _(s):
            gain_copy(partner(me, s, n)).wait_send()

        @pl.loop(1, n)
        def _(s):
            dev = partner(me, s, n)
            for a in range(3):
                back_copy(a, dev).wait_send()

    wait_back(1)


def store(*refs):
    count = len(refs) // 2
    sems = refs[-1]
    copies = [
        pltpu.make_async_copy(refs[i], refs[count + i], sems.at[i]) for i in range(count)
    ]
    for copy in copies:
        copy.start()
    for copy in copies:
        copy.wait()


def solution(mesh):
    n, n_uly = mesh.shape["blk"], mesh.shape["uly"]

    def local(q_raw, k_raw, values, out_grad, q_gain, k_gain):
        rows, heads, width = q_raw.shape
        total = n * rows
        vmem = pl.BlockSpec(memory_space=pltpu.VMEM)
        first = [jnp.transpose(x, (1, 0, 2)) for x in (k_raw, values, q_raw, out_grad)]
        out_block = jax.ShapeDtypeStruct((heads, rows, width), bf16)
        hbm = pl.BlockSpec(memory_space=pltpu.HBM)
        gain_block = jax.ShapeDtypeStruct((2, width), f32)
        shapes = (out_block,) * 3 + (gain_block,) * 2
        held = tuple(pltpu.VMEM(x.shape, x.dtype) for x in shapes)
        results = pl.pallas_call(
            functools.partial(kernel, n, n_uly, heads, rows),
            out_shape=held,
            in_specs=[hbm] * 6,
            out_specs=(vmem,) * 5,
            scratch_shapes=[pltpu.VMEM((heads, rows, width), bf16)] * 4
            + [pltpu.VMEM((total, width), bf16)] * 5
            + [pltpu.VMEM((width, total), bf16)]
            + [pltpu.VMEM((total, width), f32)] * 2
            + [pltpu.VMEM((total, width), bf16)] * 3
            + [pltpu.VMEM((total, CHUNK), f32)] * 2
            + [pltpu.VMEM((total, CHUNK), bf16)] * 3
            + [pltpu.VMEM((total // LANES, CHUNK), f32)] * 4
            + [
                pltpu.VMEM((2, width), f32),
                pltpu.VMEM((2, width), f32),
                pltpu.VMEM((4, width), f32),
                pltpu.VMEM((heads, 4, width), f32),
                pltpu.VMEM((4, width), f32),
                pltpu.VMEM((n_uly, 4, width), f32),
                pltpu.SemaphoreType.DMA((6,)),
                pltpu.SemaphoreType.DMA((4, n)),
                pltpu.SemaphoreType.DMA((4, n)),
                pltpu.SemaphoreType.DMA((3, n)),
                pltpu.SemaphoreType.DMA((3, heads)),
                pltpu.SemaphoreType.DMA((n,)),
                pltpu.SemaphoreType.DMA((heads,)),
                pltpu.SemaphoreType.DMA((n_uly,)),
                pltpu.SemaphoreType.DMA((n_uly,)),
                pltpu.SemaphoreType.REGULAR,
            ],
            compiler_params=pltpu.CompilerParams(
                collective_id=0, has_side_effects=True, vmem_limit_bytes=KERNEL_VMEM
            ),
        )(*[pltpu.with_memory_space_constraint(x, pltpu.HBM) for x in (*first, q_gain, k_gain)])
        dq, dk, dv, q_total, k_total = pl.pallas_call(
            store,
            out_shape=shapes,
            in_specs=[vmem] * 5,
            out_specs=(hbm,) * 5,
            scratch_shapes=[pltpu.SemaphoreType.DMA((5,))],
            compiler_params=pltpu.CompilerParams(vmem_limit_bytes=STORE_VMEM),
        )(*results)
        back = [jnp.transpose(x, (1, 0, 2)) for x in (dq, dk, dv)]
        return (*back, q_total, k_total)

    placed = (P("blk", "uly", None),) * 4 + (P(), P())
    return jax.shard_map(
        local,
        mesh=mesh,
        in_specs=placed,
        out_specs=(P("blk", "uly", None),) * 3 + (P(), P()),
        check_vma=False,
    )
```
